128 devices in a mesh: dom: 128 (over x, z, y, core).
Axes of the slice: x: 4, y: 4, z: 4, core: 2. Of those that a mesh axis runs over, the one named last changes fastest.
Arguments:
- modal_dofs: float32 [35, 9, 32768], P(None, None, 'dom'), may hold values from -6 to 6
- jacobian: float32 [3, 32768], P(None, 'dom'), may hold values from 0.2 to 0.8
- face_area: float32 [4, 32768], P(None, 'dom'), may hold values from 0.1 to 0.4
- cluster_id: int32 [32768], P('dom'), may hold values from 0 to 1
- target_slot: int32 [32768], P('dom'), may hold values from 0 to 383, as said below
- ghost_slots: int32 [128, 8, 6], P('dom'), may hold values from 0 to 383
- face_neighbours: int32 [4, 49152], P(None, 'dom'), may hold values from 0 to 431, as said below
- stiffness: float32 [3, 35, 35], replicated, may hold values from -1 to 1
- star_matrix: float32 [3, 9, 9], replicated, may hold values from -2 to 2
- face_minus: float32 [4, 35, 35], replicated, may hold values from -1 to 1
- face_plus: float32 [4, 35, 35], replicated, may hold values from -1 to 1
- solver_minus: float32 [4, 9, 9], replicated, may hold values from -2 to 2
- solver_plus: float32 [4, 9, 9], replicated, may hold values from -2 to 2
Outputs:
- updated: float32 [35, 9, 32768], P(None, None, 'dom')
The draws below stay inside these ranges and needn't reach their ends.
Inputs may be any that keep to these rules, and one draw needn't show every extreme that they name: `target_slot`: within the 256 elements of one block the values are distinct. One owner, the same for every block, receives 3 elements from every block. `face_neighbours`: values from 384 on address the ghost table of 48 entries.
All inputs are finite; a program needn't handle non-finite values.
Results may differ from the reference program's by a relative error of at most 0.0003.
Values sent between devices are 32-bit elements; how exact they have to be, the bound alone decides.
No kernel may reach another device: no remote copies, remote signals or barrier semaphores. Data moves between devices by JAX's collectives and lax.ppermute only.
A program may use at most 64 MiB of HBM per device.

```python
import math
import jax
import jax.numpy as jnp
from jax import lax

ORDER = 5
MODES = 35
QUANT = 9
NEIGH = 8
E_DEV = 256
CAP = 3
SLOTS = 384
GHOSTS = 6
ELEMS = 32768
N_DOM = 128


def draw_target_slot(key, part):
    slot_total = N_DOM * CAP
    full_owner = jax.random.randint(jax.random.fold_in(key, 11), (), 0, N_DOM)
    block_keys = jax.random.split(jax.random.fold_in(key, 12), N_DOM)

    def one_block(block_key):
        order_key = jax.random.fold_in(block_key, 1)
        assign_key = jax.random.fold_in(block_key, 2)
        ranking = jax.random.permutation(order_key, slot_total).astype(jnp.int32)
        slot_ids = jnp.arange(slot_total, dtype=jnp.int32)
        priority = jnp.where(slot_ids // CAP == full_owner, -1, ranking)
        chosen = jnp.argsort(priority, stable=True)[:E_DEV].astype(jnp.int32)
        return chosen[jax.random.permutation(assign_key, E_DEV)]
    return jax.vmap(one_block)(block_keys).reshape(-1).astype(jnp.int32)


def draw_face_neighbours(key, part):
    total = N_DOM * SLOTS
    local_key = jax.random.fold_in(key, 21)
    ghost_key = jax.random.fold_in(key, 22)
    pick_key = jax.random.fold_in(key, 23)
    local_part = jax.random.randint(local_key, (4, total), 0, SLOTS)
    ghost_part = SLOTS + jax.random.randint(ghost_key, (4, total), 0, NEIGH * GHOSTS)
    remote_face = jax.random.randint(pick_key, (4, total), 0, 8) == 0
    return jnp.where(remote_face, ghost_part, local_part).astype(jnp.int32)


def set_ends(values, stream_key, smallest, top_value):
    shape = values.shape
    place = [jax.random.randint(jax.random.fold_in(stream_key, axis), (), 0, shape[axis]) for axis in range(len(shape))]
    values = values.at[tuple(place)].set(smallest)
    longest = shape.index(max(shape))
    place[longest] = (place[longest] + 1) % shape[longest]
    return values.at[tuple(place)].set(top_value)


def block_scale(key, shape, shards, low, top_value):
    def one(dim, shards_of):
        draws = jax.random.uniform(jax.random.fold_in(jax.random.fold_in(key, 6), dim), (shards_of,), jnp.float32, low / len(shards), top_value / len(shards))
        return jnp.repeat(jnp.exp(draws), shape[dim] // shards_of).reshape((-1,) + (1,) * (len(shape) - dim - 1))

    level = one(*shards[0])
    for cut in shards[1:]:
        level = level * one(*cut)
    return level


def normal_values(key, extent, width, reach, cuts=(), kind=jnp.bfloat16):
    entries = width * jax.random.normal(key, extent, jnp.float32)
    if cuts:
        entries = entries * block_scale(key, extent, cuts, -0.22, 0.18)
    return jnp.clip(entries, -reach, reach).astype(kind)


def setup_inputs(seed: int = 0) -> dict:
    key_list = jax.random.split(jax.random.key(seed), 14)
    modal_dofs = normal_values(key_list[0], (MODES, QUANT, ELEMS), 1.0, 6.0, ((2, 128),), jnp.float32)
    jacobian = jnp.clip(jnp.exp(math.log(0.8) - 1.3862944 * jax.random.uniform(key_list[1], (3, ELEMS), jnp.float32) ** block_scale(key_list[1], (3, ELEMS), ((1, 128),), -0.2, 0.2)), 0.2, 0.8)
    face_area = jnp.clip(jnp.exp(math.log(0.4) - 1.3862944 * jax.random.uniform(key_list[2], (4, ELEMS), jnp.float32) ** block_scale(key_list[2], (4, ELEMS), ((1, 128),), -0.2, 0.2)), 0.1, 0.4)
    cluster_id = set_ends(jax.random.randint(key_list[3], (ELEMS,), 0, 2), jax.random.fold_in(key_list[3], 1), 0, 1).astype(jnp.int32)
    target_slot = draw_target_slot(jax.random.fold_in(key_list[13], 71), 0)
    ghost_slots = set_ends(jax.random.randint(key_list[5], (N_DOM, NEIGH, GHOSTS), 0, SLOTS), jax.random.fold_in(key_list[5], 1), 0, SLOTS - 1).astype(jnp.int32)
    face_neighbours = draw_face_neighbours(jax.random.fold_in(key_list[13], 71), 0)
    stiffness = normal_values(key_list[7], (3, MODES, MODES), MODES ** -0.5, 1.0, (), jnp.float32)
    star_matrix = normal_values(key_list[8], (3, QUANT, QUANT), QUANT ** -0.5, 2.0, (), jnp.float32)
    face_minus = normal_values(key_list[9], (4, MODES, MODES), MODES ** -0.5, 1.0, (), jnp.float32)
    face_plus = normal_values(key_list[10], (4, MODES, MODES), MODES ** -0.5, 1.0, (), jnp.float32)
    solver_minus = normal_values(key_list[11], (4, QUANT, QUANT), QUANT ** -0.5, 2.0, (), jnp.float32)
    solver_plus = normal_values(key_list[12], (4, QUANT, QUANT), QUANT ** -0.5, 2.0, (), jnp.float32)
    return {"modal_dofs": modal_dofs, "jacobian": jacobian, "face_area": face_area, "cluster_id": cluster_id, "target_slot": target_slot, "ghost_slots": ghost_slots, "face_neighbours": face_neighbours, "stiffness": stiffness, "star_matrix": star_matrix, "face_minus": face_minus, "face_plus": face_plus, "solver_minus": solver_minus, "solver_plus": solver_plus}


exact_precision = lax.Precision.HIGHEST
neighbour_steps = (1, -1, 2, -2, 3, -3, 4, -4)


def coefficients(lower_end, upper_end):
    return [(upper_end ** (degree + 1) - lower_end ** (degree + 1)) / math.factorial(degree + 1) for degree in range(ORDER)]


def derive(start_state, scaling, stiffness, star_matrix):
    taylor_terms = [start_state]
    current = start_state
    for degree in range(ORDER - 1):
        rotated = jnp.einsum('cmn,mqs->cnqs', stiffness, current, precision=exact_precision)
        rotated = rotated * scaling[:, None, None, :]
        current = -jnp.einsum('cnqs,cqp->nps', rotated, star_matrix, precision=exact_precision)
        taylor_terms.append(current)
    return taylor_terms


def combine_terms(taylor_terms, factors):
    summed = taylor_terms[0] * factors[0]
    for series_term, factor in zip(taylor_terms[1:], factors[1:]):
        summed = summed + series_term * factor
    return summed


def increment(values, beside, scaling, face_scale, stiffness, star_matrix, face_minus, face_plus, solver_minus, solver_plus):
    volume = jnp.einsum('cnm,mqs->cnqs', stiffness, values, precision=exact_precision) * scaling[:, None, None, :]
    volume = jnp.einsum('cnqs,cqp->nps', volume, star_matrix, precision=exact_precision)
    local_flux = jnp.einsum('fnm,mqs->fnqs', face_minus, values, precision=exact_precision) * face_scale[:, None, None, :]
    local_flux = jnp.einsum('fnqs,fqp->nps', local_flux, solver_minus, precision=exact_precision)
    remote = jnp.einsum('fnm,mqfs->fnqs', face_plus, beside, precision=exact_precision) * face_scale[:, None, None, :]
    remote = jnp.einsum('fnqs,fqp->nps', remote, solver_plus, precision=exact_precision)
    return volume - local_flux - remote


def reference(modal_dofs, jacobian, face_area, cluster_id, target_slot, ghost_slots, face_neighbours, stiffness, star_matrix, face_minus, face_plus, solver_minus, solver_plus):
    slot_total = N_DOM * SLOTS
    element = jnp.arange(ELEMS, dtype=jnp.int32)
    block_id = element // E_DEV
    owner_index = (target_slot // CAP) * SLOTS + block_id * CAP + target_slot % CAP
    owned = jnp.zeros((MODES, QUANT, slot_total), jnp.float32).at[:, :, owner_index].set(modal_dofs)
    owned_jac = jnp.zeros((3, slot_total), jnp.float32).at[:, owner_index].set(jacobian)
    owned_area = jnp.zeros((4, slot_total), jnp.float32).at[:, owner_index].set(face_area)
    weight = jnp.zeros((slot_total,), jnp.float32).at[owner_index].set(1.0 + cluster_id.astype(jnp.float32))
    slot_id = jnp.arange(slot_total, dtype=jnp.int32)
    owner_id = slot_id // SLOTS
    step_table = jnp.array(neighbour_steps, dtype=jnp.int32)
    beyond = jnp.maximum(face_neighbours - SLOTS, 0).astype(jnp.int32)
    neighbour_id = jnp.minimum(beyond // GHOSTS, NEIGH - 1).astype(jnp.int32)
    peer_id = ((owner_id[None, :] - step_table[neighbour_id]) % N_DOM).astype(jnp.int32)
    remote_slot = ghost_slots[peer_id, neighbour_id, beyond % GHOSTS]
    source = jnp.where(face_neighbours < SLOTS, owner_id[None, :] * SLOTS + face_neighbours, peer_id * SLOTS + remote_slot).astype(jnp.int32)
    positions = jnp.arange(N_DOM, dtype=jnp.int32)

    def spread(stacked):
        return jnp.moveaxis(stacked, 0, 2).reshape(MODES, QUANT, slot_total)

    def first_section(position):
        offset = position * SLOTS
        start_state = lax.dynamic_slice_in_dim(owned, offset, SLOTS, 2)
        scaling = lax.dynamic_slice_in_dim(owned_jac, offset, SLOTS, 1)
        taylor_terms = derive(start_state, scaling, stiffness, star_matrix)
        return combine_terms(taylor_terms, coefficients(0.0, 1.0)), combine_terms(taylor_terms, coefficients(1.0, 2.0))

    first_part, later_part = lax.map(first_section, positions)
    first_part = spread(first_part)
    later_part = spread(later_part)

    def update_section(values, current):
        def update_owner(position):
            offset = position * SLOTS
            block_values = lax.dynamic_slice_in_dim(values, offset, SLOTS, 2)
            picked = lax.dynamic_slice_in_dim(source, offset, SLOTS, 1).reshape(-1)
            beside = jnp.take(values, picked, axis=2).reshape(MODES, QUANT, 4, SLOTS)
            scaling = lax.dynamic_slice_in_dim(owned_jac, offset, SLOTS, 1)
            face_scale = lax.dynamic_slice_in_dim(owned_area, offset, SLOTS, 1)
            occupied = (lax.dynamic_slice_in_dim(weight, offset, SLOTS, 0) > 0.5).astype(jnp.float32)
            change = increment(block_values, beside, scaling, face_scale, stiffness, star_matrix, face_minus, face_plus, solver_minus, solver_plus)
            return lax.dynamic_slice_in_dim(current, offset, SLOTS, 2) + occupied * change
        return spread(lax.map(update_owner, positions))

    middle = update_section(first_part, owned)

    def second_section(position):
        offset = position * SLOTS
        start_state = lax.dynamic_slice_in_dim(middle, offset, SLOTS, 2)
        scaling = lax.dynamic_slice_in_dim(owned_jac, offset, SLOTS, 1)
        fresh_part = combine_terms(derive(start_state, scaling, stiffness, star_matrix), coefficients(0.0, 1.0))
        slow_mask = lax.dynamic_slice_in_dim(weight, offset, SLOTS, 0) > 1.5
        return jnp.where(slow_mask[None, None, :], lax.dynamic_slice_in_dim(later_part, offset, SLOTS, 2), fresh_part)

    second = spread(lax.map(second_section, positions))
    final_state = update_section(second, middle)
    return final_state[:, :, owner_index]
```

```python
import math

import jax
import jax.numpy as jnp
from jax import lax
from jax.experimental import pallas as pl
from jax.experimental.pallas import tpu as pltpu
from jax.sharding import PartitionSpec as P

ORDER = 5
MODES = 35
QUANT = 9
FEAT = MODES * QUANT
ROWS = 320
BLOCK = 256
DEVS = 128
CAP = 3
SLOTS = 384
STRIDE = 336
CHUNK = 1024
GHOSTS = 6
NEIGH = 8
STEPS = (1, -1, 2, -2, 3, -3, 4, -4)
F32 = jnp.float32
BF16 = jnp.bfloat16
FULL = 67043328


def weights_of(lower, upper):
    return [(upper ** (k + 1) - lower ** (k + 1)) / math.factorial(k + 1) for k in range(ORDER)]


def dot(a, b):
    return jnp.dot(a, b, preferred_element_type=F32)


def split2(x):
    high = x.astype(BF16)
    return high, (x - high.astype(F32)).astype(BF16)


def split3(x):
    high = x.astype(BF16)
    rest = x - high.astype(F32)
    mid = rest.astype(BF16)
    return high, mid, (rest - mid.astype(F32)).astype(BF16)


def dot3(a, b, dims=None):
    total = None
    for part in split3(a):
        if dims is None:
            term = dot(part, b)
        else:
            term = lax.dot_general(part, b, (dims, ((), ())), preferred_element_type=F32)
        total = term if total is None else total + term
    return total


def product(a_high, a_low, b_high, b_low):
    return dot(a_high, b_high) + dot(a_low, b_high) + dot(a_high, b_low)


def iota(shape, dim):
    return lax.broadcasted_iota(jnp.int32, shape, dim)


def onehot(condition):
    return jnp.where(condition, 1.0, 0.0).astype(BF16)


def pack_rows(stage, out_ref):
    for k in range(8):
        out_ref[pl.ds(k, DEVS, stride=8), :] = stage[128 * k : 128 * k + 128, :].T


def unpack_rows(recv_ref, stage):
    for k in range(8):
        stage[128 * k : 128 * k + 128, :] = recv_ref[pl.ds(k, DEVS, stride=8), :].T


def scatter_kernel(modal, jac, area, cluster, target, out, cells, values, stage, kinds, places, done):
    copies = [
        pltpu.make_async_copy(modal, cells, done.at[0]),
        pltpu.make_async_copy(jac, values.at[0:3, :], done.at[1]),
        pltpu.make_async_copy(area, values.at[3:7, :], done.at[2]),
        pltpu.make_async_copy(cluster, kinds, done.at[3]),
        pltpu.make_async_copy(target, places, done.at[4]),
    ]
    for copy in copies:
        copy.start()
    for copy in copies:
        copy.wait()
    values[7:8, :] = 1.0 + kinds[...].astype(F32)
    values[320:328, :] = jnp.zeros((8, BLOCK), F32)
    for q in range(QUANT):
        values[8 + MODES * q : 8 + MODES * (q + 1), :] = cells[q]
    slot = iota((DEVS, BLOCK), 0) * CAP
    wanted = places[...]
    stage[CAP * STRIDE :, :] = jnp.zeros((CHUNK - CAP * STRIDE, DEVS), F32)
    parts = split3(values[...])
    for t in range(CAP):
        hot = onehot(slot + t == wanted)
        total = None
        for part in parts:
            term = lax.dot_general(part, hot, (((1,), (1,)), ((), ())), preferred_element_type=F32)
            total = term if total is None else total + term
        stage[STRIDE * t : STRIDE * t + 328, :] = total
        stage[STRIDE * t + 328 : STRIDE * (t + 1), :] = jnp.zeros((8, DEVS), F32)
    pack_rows(stage, out)


def gather_kernel(recv, target, out, stage):
    unpack_rows(recv, stage)
    wanted = target[...]
    slot = iota((DEVS, BLOCK), 0) * CAP
    total = None
    for t in range(CAP):
        part = stage[STRIDE * t + 8 : STRIDE * t + 8 + ROWS, :]
        term = dot3(part, onehot(slot + t == wanted))
        total = term if total is None else total + term
    for q in range(QUANT):
        out[q] = total[MODES * q : MODES * (q + 1), :]


def expand_family(mode_in, flux_in, first, count, sign, high, low, at, stage):
    width = count * ROWS
    col = iota((8, width), 1)
    op = jnp.zeros_like(col)
    for c in range(1, count):
        op = op + jnp.where(col >= c * ROWS, 1, 0)
    inner = col - op * ROWS
    quant = (inner * 1873) >> 16
    mode = inner - quant * MODES
    valid = inner < FEAT
    mode_code = jnp.where(valid, op * 128 + mode, -1)[0:1]
    quant_code = jnp.where(valid, op * 128 + quant, -1)[0:1]
    row = iota((count * 128, width), 0)
    modes = jnp.concatenate([mode_in[first + c] for c in range(count)], axis=1)
    fluxes = jnp.concatenate([flux_in[first + c] for c in range(count)], axis=1)
    spread = dot3(modes, onehot(row == mode_code)) * sign
    scale = dot3(fluxes, onehot(row == quant_code))
    for p in range(QUANT):
        stage[MODES * p : MODES * (p + 1), 0:width] = spread[0:MODES, :] * scale[p : p + 1, :]
    stage[FEAT:ROWS, 0:width] = jnp.zeros((ROWS - FEAT, width), F32)
    a_high, a_low = split2(stage[:, 0:width])
    high[:, at : at + width] = a_high
    low[:, at : at + width] = a_low


def operator_kernel(mode_in, flux_in, faces, d_high, d_low, c_high, c_low, b_high, b_low, order,
    stage, dh, dl, bh, bl, ch, cl, moved, done,
):
    expand_family(mode_in, flux_in, 0, 3, -1.0, dh, dl, 0, stage)
    copies = fetch([(dh, d_high), (dl, d_low)], done)
    expand_family(mode_in, flux_in, 10, 4, -1.0, bh, bl, 0, stage)
    copies += fetch([(bh, b_high), (bl, b_low)], done, 2)
    expand_family(mode_in, flux_in, 3, 3, 1.0, ch, cl, 0, stage)
    expand_family(mode_in, flux_in, 6, 4, -1.0, ch, cl, 3 * ROWS, stage)
    copies += fetch([(ch, c_high), (cl, c_low)], done, 4)
    value = faces[...]
    digits = jnp.concatenate([value >> 4, value & 15], axis=0).astype(F32).astype(BF16)
    row = iota((SLOTS, SLOTS), 0)
    col = iota((SLOTS, SLOTS), 1)
    swapped = dot(digits, onehot(row == (col & 127) * CAP + (col >> 7))).astype(jnp.int32)
    moved[...] = swapped[0:4, :] * 16 + swapped[4:8, :]
    copies += fetch([(moved, order)], done, 6)
    for copy in copies:
        copy.wait()


def taylor(start, extras, d_high, d_low, x_high, x_low, factor_sets):
    sums = [start * factors[0] for factors in factor_sets]
    current = start
    for k in range(1, ORDER):
        for c in range(3):
            high, low = split2(current * extras[c : c + 1, :])
            x_high[ROWS * c : ROWS * (c + 1), :] = high
            x_low[ROWS * c : ROWS * (c + 1), :] = low
        current = product(d_high[...], d_low[...], x_high[...], x_low[...])
        sums = [s + current * factors[k] for s, factors in zip(sums, factor_sets)]
    return sums


def send_ghosts(value, picks, owner, out):
    out[...] = jnp.zeros(out.shape, F32)
    slot = iota((SLOTS, 128), 0)
    slot = (slot & 127) * CAP + (slot >> 7)
    base = onehot(slot == picks[0:1, :])
    rest = jnp.concatenate([onehot(slot == picks[k : k + 1, :]) for k in range(1, 5)], axis=1)
    main = dot3(value[0:256, :], base)
    tail = dot3(value[256:320, :], rest)
    first = (main[0:128, :] + jnp.concatenate([tail[:, 0:128], tail[:, 128:256]], axis=0)).T
    second = (main[128:256, :] + jnp.concatenate([tail[:, 256:384], tail[:, 384:512]], axis=0)).T
    spot = owner & 7
    for b, step in enumerate(STEPS):
        goal = spot + step
        outside = jnp.where((goal < 0) | (goal > 7), 16, 0)
        place = ((goal + 8) & 7) * 32 + outside
        out[pl.ds(pl.multiple_of(place, 16), 8), :] = first[8 * b : 8 * b + 8, :]
        out[pl.ds(pl.multiple_of(place + 8, 8), 8), :] = second[8 * b : 8 * b + 8, :]


def read_ghosts(near, above, below, owner):
    firsts, seconds = [], []
    spot = owner & 7
    for step in STEPS:
        origin = spot - step
        inside = (origin >= 0) & (origin <= 7)
        place = pl.multiple_of(((origin + 8) & 7) * 32, 32)
        far = pl.multiple_of((origin & 3) * 16, 16)
        other = above if step > 0 else below
        firsts.append(jnp.where(inside, near[pl.ds(place, 8), :], other[pl.ds(far, 8), :]))
        seconds.append(jnp.where(inside, near[pl.ds(place + 8, 8), :], other[pl.ds(far + 8, 8), :]))
    blank = jnp.zeros((64, 128), F32)
    first = jnp.concatenate(firsts + [blank], axis=0).T
    second = jnp.concatenate(seconds + [blank], axis=0).T
    row = iota((128, 128), 0)
    col = iota((128, 128), 1)
    part = col & 7
    group = col - part
    halves = [first[0:64, :], first[64:128, :], second[0:64, :], second[64:128, :]]
    places = [((0, 6), (2, 7)), ((1, 6), (3, 7)), ((4, 6),), ((5, 6),)]
    tail = None
    for half, moves in zip(halves, places):
        hit = None
        for ghost, spot in moves:
            one = (part == ghost) & (row == group + spot)
            hit = one if hit is None else hit | one
        term = dot3(half, onehot(hit))
        tail = term if tail is None else tail + term
    return jnp.concatenate([first, second, tail], axis=0)


def remote_flux(value, ghosts, extras, faces, b_high, b_low, y_high, y_low, copies):
    high, low = split2(jnp.concatenate([value, ghosts], axis=1))
    row = iota((512, 128), 0)
    beyond = row - SLOTS
    local = (row & 127) * CAP + (row >> 7)
    spot = beyond & 7
    ghost = jnp.where((spot < GHOSTS) & (beyond < 64), SLOTS + (beyond >> 3) * GHOSTS + spot, -1)
    code = jnp.where(row < SLOTS, local, ghost)
    for f in range(4):
        hot = jnp.concatenate(
            [onehot(code == faces[f : f + 1, 128 * k : 128 * (k + 1)]) for k in range(3)], axis=1
        )
        picked = (dot(high, hot) + dot(low, hot)) * extras[3 + f : 4 + f, :]
        p_high, p_low = split2(picked)
        y_high[ROWS * f : ROWS * (f + 1), :] = p_high
        y_low[ROWS * f : ROWS * (f + 1), :] = p_low
    for copy in copies:
        copy.wait()
    return product(b_high[...], b_low[...], y_high[...], y_low[...])


def fetch(pairs, done, base=0):
    copies = [pltpu.make_async_copy(src, dst, done.at[base + k]) for k, (src, dst) in enumerate(pairs)]
    for copy in copies:
        copy.start()
    return copies


def occupied(extras):
    return jnp.where(extras[7:8, :] > 0.5, 1.0, 0.0)


def start_kernel(owner, recv, picks, d_high, d_low, state, extras, first, later, ghosts, stage, dh, dl, x_high, x_low, done):
    copies = fetch([(d_high, dh), (d_low, dl)], done)
    unpack_rows(recv, stage)
    for t in range(CAP):
        extras[:, 128 * t : 128 * (t + 1)] = stage[STRIDE * t : STRIDE * t + 8, :]
        state[:, 128 * t : 128 * (t + 1)] = stage[STRIDE * t + 8 : STRIDE * t + 8 + ROWS, :]
    for copy in copies:
        copy.wait()
    one, two = taylor(
        state[...], extras, dh, dl, x_high, x_low, [weights_of(0.0, 1.0), weights_of(1.0, 2.0)]
    )
    first[...] = one
    later[...] = two
    send_ghosts(first, picks, owner[0], ghosts)


def local_kernel(state, value, extras, c_high, c_low, out, z_high, z_low):
    for k in range(7):
        high, low = split2(value[...] * extras[k : k + 1, :])
        z_high[ROWS * k : ROWS * (k + 1), :] = high
        z_low[ROWS * k : ROWS * (k + 1), :] = low
    change = product(c_high[...], c_low[...], z_high[...], z_low[...])
    out[...] = state[...] + occupied(extras) * change


def middle_kernel(
    owner, near, above, below, partial, first, later, extras, faces, picks, d_high, d_low, b_high, b_low,
    middle, second, ghosts, dh, dl, bh, bl, x_high, x_low, y_high, y_low, done,
):
    copies = fetch([(b_high, bh), (b_low, bl), (d_high, dh), (d_low, dl)], done)
    table = read_ghosts(near, above, below, owner[0])
    flux = remote_flux(first[...], table, extras, faces, bh, bl, y_high, y_low, copies[0:2])
    for copy in copies[2:4]:
        copy.wait()
    middle[...] = partial[...] + occupied(extras) * flux
    (fresh,) = taylor(middle[...], extras, dh, dl, x_high, x_low, [weights_of(0.0, 1.0)])
    second[...] = jnp.where(extras[7:8, :] > 1.5, later[...], fresh)
    send_ghosts(second, picks, owner[0], ghosts)


def final_kernel(
    owner, near, above, below, partial, second, extras, faces, b_high, b_low, out, stage, bh, bl, y_high, y_low, done
):
    copies = fetch([(b_high, bh), (b_low, bl)], done)
    table = read_ghosts(near, above, below, owner[0])
    flux = remote_flux(second[...], table, extras, faces, bh, bl, y_high, y_low, copies)
    final = partial[...] + occupied(extras) * flux
    stage[...] = jnp.zeros((CHUNK, DEVS), F32)
    for t in range(CAP):
        stage[STRIDE * t + 8 : STRIDE * t + 8 + ROWS, :] = final[:, 128 * t : 128 * (t + 1)]
    pack_rows(stage, out)


def shape(*dims, dtype=F32):
    return jax.ShapeDtypeStruct(dims, dtype)


def call(kernel, name, outs, scratch, flops, operands, spaces="", out_spaces="", limit=16 * 1024 * 1024):
    kinds = {"s": pltpu.SMEM, "v": pltpu.VMEM, "h": pltpu.HBM}
    spaces = spaces.ljust(len(operands), "v")
    flat = jax.tree.leaves(outs)
    out_specs = [pl.BlockSpec(memory_space=kinds[k]) for k in out_spaces.ljust(len(flat), "v")]
    moved = sum(math.prod(o.shape) * 4 for o in operands)
    return pl.pallas_call(
        kernel,
        name=name,
        out_shape=outs,
        in_specs=[pl.BlockSpec(memory_space=kinds[k]) for k in spaces],
        out_specs=out_specs if isinstance(outs, list) else out_specs[0],
        scratch_shapes=scratch,
        cost_estimate=pl.CostEstimate(flops=flops, bytes_accessed=moved, transcendentals=0),
        compiler_params=pltpu.CompilerParams(vmem_limit_bytes=limit),
    )(*operands)


def vmem(*dims, dtype=F32):
    return pltpu.VMEM(dims, dtype)


def exchange(rows, per):
    cube = rows.reshape(DEVS, per, 128)
    return lax.all_to_all(cube, "dom", split_axis=0, concat_axis=0, tiled=True).reshape(DEVS * per, 128)


def swap_ghosts(rows):
    groups = [list(range(8 * k, 8 * k + 8)) for k in range(DEVS // 8)]
    cube = rows.reshape(8, 32, 128)
    near = lax.all_to_all(cube, "dom", split_axis=0, concat_axis=0, axis_index_groups=groups, tiled=True)
    up = [(i, (i + 8) % DEVS) for i in range(DEVS)]
    down = [((i + 8) % DEVS, i) for i in range(DEVS)]
    above = lax.ppermute(near[4:8, 16:32].reshape(64, 128), "dom", up)
    below = lax.ppermute(near[0:4, 16:32].reshape(64, 128), "dom", down)
    return near.reshape(256, 128), above, below


def local(
    modal_dofs, jacobian, face_area, cluster_id, target_slot, ghost_slots, face_neighbours,
    stiffness, star_matrix, face_minus, face_plus, solver_minus, solver_plus,
):
    owner = lax.axis_index("dom").astype(jnp.int32).reshape(1)
    target = target_slot.reshape(1, BLOCK)
    sent = call(
        scatter_kernel, "scatter", shape(CHUNK, DEVS),
        [
            vmem(QUANT, MODES, BLOCK), vmem(328, BLOCK), vmem(CHUNK, DEVS),
            vmem(1, BLOCK, dtype=jnp.int32), vmem(1, BLOCK, dtype=jnp.int32), pltpu.SemaphoreType.DMA((5,)),
        ],
        10**8,
        (jnp.transpose(modal_dofs, (1, 0, 2)), jacobian, face_area, cluster_id.reshape(1, BLOCK), target),
        "hhhhh", "", FULL,
    )
    received = exchange(sent, 8)

    modes = jnp.concatenate([jnp.transpose(stiffness, (0, 2, 1)), stiffness, face_minus, face_plus], axis=0)
    fluxes = jnp.concatenate([star_matrix, star_matrix, solver_minus, solver_plus], axis=0)
    modes = jnp.pad(modes, ((0, 0), (0, 48 - MODES), (0, 128 - MODES)))
    fluxes = jnp.pad(jnp.transpose(fluxes, (0, 2, 1)), ((0, 0), (0, 16 - QUANT), (0, 128 - QUANT)))
    sizes = [3 * ROWS, 7 * ROWS, 4 * ROWS]
    d_high, d_low, c_high, c_low, b_high, b_low, faces = call(
        operator_kernel, "operators",
        [shape(ROWS, s, dtype=BF16) for s in sizes for _ in range(2)] + [shape(4, SLOTS, dtype=jnp.int32)],
        [vmem(ROWS, 4 * ROWS)]
        + [vmem(ROWS, k * ROWS, dtype=BF16) for k in (3, 3, 4, 4, 7, 7)]
        + [vmem(4, SLOTS, dtype=jnp.int32), pltpu.SemaphoreType.DMA((7,))],
        10**9, (modes, fluxes, face_neighbours), "", "hhhhhhh", FULL,
    )
    wanted = ghost_slots[0]
    none = jnp.full((NEIGH, 1), -1, jnp.int32)
    wide = jnp.full((NEIGH, 6), -1, jnp.int32)

    def lanes(*columns):
        table = jnp.concatenate(columns, axis=1).reshape(1, 64)
        return jnp.concatenate([table, jnp.full((1, 64), -1, jnp.int32)], axis=1)

    picks = jnp.concatenate(
        [
            lanes(wanted, none, none),
            lanes(wide, wanted[:, 0:1], wanted[:, 2:3]),
            lanes(wide, wanted[:, 1:2], wanted[:, 3:4]),
            lanes(wide, wanted[:, 4:5], none),
            lanes(wide, wanted[:, 5:6], none),
            jnp.full((3, 128), -1, jnp.int32),
        ],
        axis=0,
    )
    d_scratch = [vmem(ROWS, 3 * ROWS, dtype=BF16)] * 2
    b_scratch = [vmem(ROWS, 4 * ROWS, dtype=BF16)] * 2
    x_scratch = [vmem(3 * ROWS, SLOTS, dtype=BF16)] * 2
    y_scratch = [vmem(4 * ROWS, SLOTS, dtype=BF16)] * 2
    z_scratch = [vmem(7 * ROWS, SLOTS, dtype=BF16)] * 2
    field = shape(ROWS, SLOTS)
    halo = shape(8 * 32, 128)
    state, extras, first, later, out1 = call(
        start_kernel, "start", [field, shape(8, SLOTS), field, field, halo],
        [vmem(CHUNK, DEVS)] + d_scratch + x_scratch + [pltpu.SemaphoreType.DMA((2,))], 10**9,
        (owner, received, picks, d_high, d_low), "svvhh",
    )
    near, above, below = swap_ghosts(out1)
    first, _ = lax.optimization_barrier((first, near))
    partial1 = call(
        local_kernel, "local1", field, z_scratch, 10**9, (state, first, extras, c_high, c_low)
    )
    middle, second, out2 = call(
        middle_kernel, "middle", [field, field, halo],
        d_scratch + b_scratch + x_scratch + y_scratch + [pltpu.SemaphoreType.DMA((4,))], 2 * 10**9,
        (owner, near, above, below, partial1, first, later, extras, faces, picks, d_high, d_low, b_high, b_low),
        "svvvvvvvvvhhhh",
    )
    near, above, below = swap_ghosts(out2)
    second, _ = lax.optimization_barrier((second, near))
    partial2 = call(
        local_kernel, "local2", field, z_scratch, 10**9, (middle, second, extras, c_high, c_low)
    )
    back = call(
        final_kernel, "final", shape(CHUNK, DEVS),
        [vmem(CHUNK, DEVS)] + b_scratch + y_scratch + [pltpu.SemaphoreType.DMA((2,))], 10**9,
        (owner, near, above, below, partial2, second, extras, faces, b_high, b_low), "svvvvvvvhh",
    )
    returned = exchange(back, 8)
    result = call(
        gather_kernel, "gather", shape(QUANT, MODES, BLOCK), [vmem(CHUNK, DEVS)], 10**8, (returned, target)
    )
    return jnp.transpose(result, (1, 0, 2))


def solution(mesh):
    placed = (
        P(None, None, "dom"), P(None, "dom"), P(None, "dom"), P("dom"), P("dom"), P("dom", None, None),
        P(None, "dom"), P(), P(), P(), P(), P(), P(),
    )
    return jax.shard_map(
        local, mesh=mesh, in_specs=placed, out_specs=P(None, None, "dom"), check_vma=False
    )
```

```python
import math

import jax
import jax.numpy as jnp
from jax import lax
from jax.experimental import pallas as pl
from jax.experimental.pallas import tpu as pltpu
from jax.sharding import PartitionSpec as P

ORDER = 5
MODES = 35
QUANT = 9
FEAT = MODES * QUANT
ROWS = 320
BLOCK = 256
DEVS = 128
CAP = 3
SLOTS = 384
STRIDE = 336
CHUNK = 1024
GHOSTS = 6
NEIGH = 8
STEPS = (1, -1, 2, -2, 3, -3, 4, -4)
F32 = jnp.float32
BF16 = jnp.bfloat16
FULL = 67043328


def weights_of(lower, upper):
    return [(upper ** (k + 1) - lower ** (k + 1)) / math.factorial(k + 1) for k in range(ORDER)]


def dot(a, b):
    return jnp.dot(a, b, preferred_element_type=F32)


def split2(x):
    high = x.astype(BF16)
    return high, (x - high.astype(F32)).astype(BF16)


def split3(x):
    high = x.astype(BF16)
    rest = x - high.astype(F32)
    mid = rest.astype(BF16)
    return high, mid, (rest - mid.astype(F32)).astype(BF16)


def dot3(a, b, dims=None):
    total = None
    for part in split3(a):
        if dims is None:
            term = dot(part, b)
        else:
            term = lax.dot_general(part, b, (dims, ((), ())), preferred_element_type=F32)
        total = term if total is None else total + term
    return total


def product(op, both):
    width = both.shape[1] // 2
    wide = dot(op[0:ROWS, :], both[...])
    return wide[:, 0:width] + wide[:, width:] + dot(op[ROWS:, :], both[:, 0:width])


def put(both, at, value):
    width = both.shape[1] // 2
    high, low = split2(value)
    both[ROWS * at : ROWS * (at + 1), 0:width] = high
    both[ROWS * at : ROWS * (at + 1), width:] = low


def owner_of(device):
    return jnp.where((device & 32) > 0, device ^ 24, device)


def iota(shape, dim):
    return lax.broadcasted_iota(jnp.int32, shape, dim)


def onehot(condition):
    return jnp.where(condition, 1.0, 0.0).astype(BF16)


def pack_rows(stage, out_ref):
    for k in range(8):
        out_ref[pl.ds(k, DEVS, stride=8), :] = stage[128 * k : 128 * k + 128, :].T


def unpack_rows(recv_ref, stage):
    for k in range(8):
        stage[128 * k : 128 * k + 128, :] = recv_ref[pl.ds(k, DEVS, stride=8), :].T


def scatter_kernel(
    modal, jac, area, cluster, target, faces, listed, out, tables, cells, values, stage, kinds, places, lists, done
):
    copies = [
        pltpu.make_async_copy(modal, cells, done.at[0]),
        pltpu.make_async_copy(jac, values.at[0:3, :], done.at[1]),
        pltpu.make_async_copy(area, values.at[3:7, :], done.at[2]),
        pltpu.make_async_copy(cluster, kinds, done.at[3]),
        pltpu.make_async_copy(target, places, done.at[4]),
        pltpu.make_async_copy(faces, tables.at[0:4, :], done.at[5]),
        pltpu.make_async_copy(listed, lists, done.at[6]),
    ]
    for copy in copies:
        copy.start()
    for copy in copies:
        copy.wait()
    tables[8:16, :] = jnp.zeros((8, SLOTS), jnp.int32)
    for i in range(GHOSTS):
        tables[8 + i : 9 + i, 0:NEIGH] = lists[i]
    values[7:8, :] = 1.0 + kinds[...].astype(F32)
    values[320:328, :] = jnp.zeros((8, BLOCK), F32)
    for q in range(QUANT):
        values[8 + MODES * q : 8 + MODES * (q + 1), :] = cells[q]
    slot = owner_of(iota((DEVS, BLOCK), 0)) * CAP
    wanted = places[...]
    stage[CAP * STRIDE :, :] = jnp.zeros((CHUNK - CAP * STRIDE, DEVS), F32)
    parts = split3(values[...])
    for t in range(CAP):
        hot = onehot(slot + t == wanted)
        total = None
        for part in parts:
            term = lax.dot_general(part, hot, (((1,), (1,)), ((), ())), preferred_element_type=F32)
            total = term if total is None else total + term
        stage[STRIDE * t : STRIDE * t + 328, :] = total
        stage[STRIDE * t + 328 : STRIDE * (t + 1), :] = jnp.zeros((8, DEVS), F32)
    pack_rows(stage, out)


def gather_kernel(recv, target, out, stage):
    unpack_rows(recv, stage)
    wanted = target[...]
    slot = owner_of(iota((DEVS, BLOCK), 0)) * CAP
    total = None
    for t in range(CAP):
        part = stage[STRIDE * t + 8 : STRIDE * t + 8 + ROWS, :]
        term = dot3(part, onehot(slot + t == wanted))
        total = term if total is None else total + term
    for q in range(QUANT):
        out[q] = total[MODES * q : MODES * (q + 1), :]


def operator_kernel(
    stiffness, minus, plus, star, solver_minus, solver_plus, d_out, c_out, b_out,
    k_in, m_in, p_in, s_in, sm_in, sp_in, tiles, square, columns, stage, b_op, c_op, loads, done,
):
    copies = fetch(
        [
            (stiffness, k_in), (minus, m_in), (plus, p_in), (star, s_in),
            (solver_minus, sm_in), (solver_plus, sp_in),
        ],
        loads,
    )
    col = iota((8, 2 * ROWS), 1)
    second = jnp.where(col >= ROWS, 1, 0)
    inner = col - second * ROWS
    quant = (inner * 1873) >> 16
    mode = inner - quant * MODES
    valid = inner < FEAT
    mode_code = jnp.where(valid, second * 128 + mode, -1)[0:1]
    quant_code = jnp.where(valid, second * 16 + quant, -512)[0:1]
    row = iota((256, 2 * ROWS), 0)
    mode_hot = onehot(row == mode_code)
    tiles[...] = jnp.zeros(tiles.shape, F32)
    square[...] = jnp.zeros(square.shape, F32)
    columns[...] = jnp.zeros(columns.shape, F32)
    for copy in copies:
        copy.wait()
    for c in range(3):
        square[0:MODES, 0:MODES] = -k_in[c]
        tiles[c] = square[...].T[0:48, :]
        tiles[3 + c, 0:MODES, 0:MODES] = k_in[c]
        columns[16 * c : 16 * c + QUANT, 0:QUANT] = s_in[:, c, :]
        columns[16 * (3 + c) : 16 * (3 + c) + QUANT, 0:QUANT] = s_in[:, c, :]
    for f in range(4):
        tiles[6 + f, 0:MODES, 0:MODES] = -m_in[:, f, :]
        tiles[10 + f, 0:MODES, 0:MODES] = -p_in[:, f, :]
        columns[16 * (6 + f) : 16 * (6 + f) + QUANT, 0:QUANT] = sm_in[:, f, :]
        columns[16 * (10 + f) : 16 * (10 + f) + QUANT, 0:QUANT] = sp_in[:, f, :]
    flux = split2(jnp.concatenate([columns[0:128, :].T[0:16, :], columns[128:256, :].T[0:16, :]], axis=1))

    def family(first, count, out):
        stage[FEAT:ROWS, :] = jnp.zeros((ROWS - FEAT, stage.shape[1]), F32)
        for k in range(0, count, 2):
            width = ROWS * min(2, count - k)
            at = first + k
            after = min(at + 1, 13)
            pair = split2(jnp.concatenate([tiles[at], tiles[after]], axis=1))
            quant_hot = onehot(row == quant_code + 16 * at)
            spread = dot(pair[0], mode_hot) + dot(pair[1], mode_hot)
            scale = dot(flux[0], quant_hot) + dot(flux[1], quant_hot)
            for p in range(QUANT):
                stage[MODES * p : MODES * (p + 1), ROWS * k : ROWS * k + width] = (
                    spread[0:MODES, 0:width] * scale[p : p + 1, 0:width]
                )
        a_high, a_low = split2(stage[:, 0 : ROWS * count])
        out[0:ROWS, :] = a_high
        out[ROWS:, :] = a_low

    family(3, 7, c_op)
    copies = fetch([(c_op, c_out)], done)
    family(10, 4, b_op)
    copies += fetch([(b_op, b_out)], done, 1)
    family(0, 3, d_out)
    for copy in copies:
        copy.wait()


def order_faces(faces):
    digits = jnp.concatenate([faces >> 4, faces & 15], axis=0).astype(F32).astype(BF16)
    from_slot = iota((SLOTS, SLOTS), 0)
    to_slot = iota((SLOTS, SLOTS), 1)
    moved = dot(digits, onehot(from_slot == (to_slot & 127) * CAP + (to_slot >> 7))).astype(jnp.int32)
    return moved[0:4, :] * 16 + moved[4:8, :]


def taylor(start, extras, d_op, pieces, factor_sets):
    cuts = [(0, 256), (256, SLOTS)]
    current = [start[:, lo:hi] for lo, hi in cuts]
    sums = [[value * factors[0] for value in current] for factors in factor_sets]
    for k in range(1, ORDER):
        for i, (lo, hi) in enumerate(cuts):
            for c in range(3):
                put(pieces[i], c, current[i] * extras[c : c + 1, lo:hi])
            current[i] = product(d_op, pieces[i])
            for total, factors in zip(sums, factor_sets):
                total[i] = total[i] + current[i] * factors[k]
    return [jnp.concatenate(total, axis=1) for total in sums]


def order_picks(listed, picks):
    value = listed
    digits = jnp.concatenate([value >> 4, value & 15], axis=0).astype(F32).astype(BF16)
    spread = dot(digits, onehot(iota((128, 128), 0) == (iota((128, 128), 1) >> 3))).astype(jnp.int32)
    spread = spread[0:8, :] * 16 + spread[8:16, :]
    lane = iota((1, 128), 1)
    part = jnp.where(lane < 64, lane & 7, 8)

    def choose(*moves):
        line = jnp.full((1, 128), -1, jnp.int32)
        for ghost, spot in moves:
            line = jnp.where(part == spot, spread[ghost : ghost + 1, :], line)
        return line

    picks[...] = jnp.full(picks.shape, -1, jnp.int32)
    picks[0:1, :] = choose(*[(i, i) for i in range(GHOSTS)])
    picks[1:2, :] = choose((0, 6), (2, 7))
    picks[2:3, :] = choose((1, 6), (3, 7))
    picks[3:4, :] = choose((4, 6))
    picks[4:5, :] = choose((5, 6))


def send_ghosts(value, picks, owner, out):
    out[...] = jnp.zeros(out.shape, F32)
    slot = iota((SLOTS, 128), 0)
    slot = (slot & 127) * CAP + (slot >> 7)
    base = onehot(slot == picks[0:1, :])
    rest = jnp.concatenate([onehot(slot == picks[k : k + 1, :]) for k in range(1, 5)], axis=1)
    main = dot3(value[0:256, :], base)
    tail = dot3(value[256:320, :], rest)
    first = (main[0:128, :] + jnp.concatenate([tail[:, 0:128], tail[:, 128:256]], axis=0)).T
    second = (main[128:256, :] + jnp.concatenate([tail[:, 256:384], tail[:, 384:512]], axis=0)).T
    spot = owner & 7
    for b, step in enumerate(STEPS):
        goal = spot + step
        outside = jnp.where((goal < 0) | (goal > 7), 16, 0)
        place = ((goal + 8) & 7) * 32 + outside
        out[pl.ds(pl.multiple_of(place, 16), 8), :] = first[8 * b : 8 * b + 8, :]
        out[pl.ds(pl.multiple_of(place + 8, 8), 8), :] = second[8 * b : 8 * b + 8, :]


def read_ghosts(near, above, below, owner):
    firsts, seconds = [], []
    spot = owner & 7
    for step in STEPS:
        origin = spot - step
        inside = (origin >= 0) & (origin <= 7)
        place = pl.multiple_of(((origin + 8) & 7) * 32, 32)
        far = pl.multiple_of((origin & 3) * 16, 16)
        other = above if step > 0 else below
        firsts.append(jnp.where(inside, near[pl.ds(place, 8), :], other[pl.ds(far, 8), :]))
        seconds.append(jnp.where(inside, near[pl.ds(place + 8, 8), :], other[pl.ds(far + 8, 8), :]))
    blank = jnp.zeros((64, 128), F32)
    first = jnp.concatenate(firsts + [blank], axis=0).T
    second = jnp.concatenate(seconds + [blank], axis=0).T
    row = iota((128, 128), 0)
    col = iota((128, 128), 1)
    part = col & 7
    group = col - part
    halves = [first[0:64, :], first[64:128, :], second[0:64, :], second[64:128, :]]
    places = [((0, 6), (2, 7)), ((1, 6), (3, 7)), ((4, 6),), ((5, 6),)]
    tail = None
    for half, moves in zip(halves, places):
        hit = None
        for ghost, spot in moves:
            one = (part == ghost) & (row == group + spot)
            hit = one if hit is None else hit | one
        term = dot3(half, onehot(hit))
        tail = term if tail is None else tail + term
    return jnp.concatenate([first, second, tail], axis=0)


def remote_flux(value, ghosts, extras, faces, b_op, both):
    high, low = split2(jnp.concatenate([value, ghosts], axis=1))
    row = iota((512, 128), 0)
    beyond = row - SLOTS
    local = (row & 127) * CAP + (row >> 7)
    spot = beyond & 7
    ghost = jnp.where((spot < GHOSTS) & (beyond < 64), SLOTS + (beyond >> 3) * GHOSTS + spot, -1)
    code = jnp.where(row < SLOTS, local, ghost)
    for f in range(4):
        hot = jnp.concatenate(
            [onehot(code == faces[f : f + 1, 128 * k : 128 * (k + 1)]) for k in range(3)], axis=1
        )
        picked = (dot(high, hot) + dot(low, hot)) * extras[3 + f : 4 + f, :]
        put(both, f, picked)
    return product(b_op, both)


def fetch(pairs, done, base=0):
    copies = [pltpu.make_async_copy(src, dst, done.at[base + k]) for k, (src, dst) in enumerate(pairs)]
    for copy in copies:
        copy.start()
    return copies


def occupied(extras):
    return jnp.where(extras[7:8, :] > 0.5, 1.0, 0.0)


def start_kernel(
    owner, recv, tables, d_op, state, extras, first, later, picks, ghosts, stage, one_piece, other_piece
):
    order_picks(tables[8:16, 0:128], picks)
    unpack_rows(recv, stage)
    for t in range(CAP):
        extras[:, 128 * t : 128 * (t + 1)] = stage[STRIDE * t : STRIDE * t + 8, :]
        state[:, 128 * t : 128 * (t + 1)] = stage[STRIDE * t + 8 : STRIDE * t + 8 + ROWS, :]
    one, two = taylor(
        state[...], extras, d_op, (one_piece, other_piece), [weights_of(0.0, 1.0), weights_of(1.0, 2.0)]
    )
    first[...] = one
    later[...] = two
    send_ghosts(first, picks, owner[0], ghosts)


def local_kernel(state, value, extras, c_op, faces, out, order, both):
    order[...] = order_faces(faces[0:4, :])
    local_terms(state, value, extras, c_op, out, both)


def local_terms(state, value, extras, c_op, out, both):
    for k in range(7):
        put(both, k, value[...] * extras[k : k + 1, :])
    change = product(c_op, both)
    out[...] = state[...] + occupied(extras) * change


def middle_kernel(
    owner, near, above, below, partial, first, later, extras, faces, picks, d_op, b_op,
    middle, second, ghosts, one_piece, other_piece, wide,
):
    table = read_ghosts(near, above, below, owner[0])
    flux = remote_flux(first[...], table, extras, faces, b_op, wide)
    middle[...] = partial[...] + occupied(extras) * flux
    (fresh,) = taylor(middle[...], extras, d_op, (one_piece, other_piece), [weights_of(0.0, 1.0)])
    second[...] = jnp.where(extras[7:8, :] > 1.5, later[...], fresh)
    send_ghosts(second, picks, owner[0], ghosts)


def final_kernel(
    owner, near, above, below, partial, second, extras, faces, b_op, out, stage, wide
):
    table = read_ghosts(near, above, below, owner[0])
    flux = remote_flux(second[...], table, extras, faces, b_op, wide)
    final = partial[...] + occupied(extras) * flux
    stage[...] = jnp.zeros((CHUNK, DEVS), F32)
    for t in range(CAP):
        stage[STRIDE * t + 8 : STRIDE * t + 8 + ROWS, :] = final[:, 128 * t : 128 * (t + 1)]
    pack_rows(stage, out)


def shape(*dims, dtype=F32):
    return jax.ShapeDtypeStruct(dims, dtype)


def call(kernel, name, outs, scratch, flops, operands, spaces="", out_spaces="", limit=16 * 1024 * 1024):
    kinds = {"s": pltpu.SMEM, "v": pltpu.VMEM, "h": pltpu.HBM}
    spaces = spaces.ljust(len(operands), "v")
    flat = jax.tree.leaves(outs)
    out_specs = [pl.BlockSpec(memory_space=kinds[k]) for k in out_spaces.ljust(len(flat), "v")]
    moved = sum(math.prod(o.shape) * 4 for o in operands)
    return pl.pallas_call(
        kernel,
        name=name,
        out_shape=outs,
        in_specs=[pl.BlockSpec(memory_space=kinds[k]) for k in spaces],
        out_specs=out_specs if isinstance(outs, list) else out_specs[0],
        scratch_shapes=scratch,
        cost_estimate=pl.CostEstimate(flops=flops, bytes_accessed=moved, transcendentals=0),
        compiler_params=pltpu.CompilerParams(vmem_limit_bytes=limit),
    )(*operands)


def vmem(*dims, dtype=F32):
    return pltpu.VMEM(dims, dtype)


def exchange(rows, per):
    cube = rows.reshape(DEVS, per, 128)
    return lax.all_to_all(cube, "dom", split_axis=0, concat_axis=0, tiled=True).reshape(DEVS * per, 128)


def device_of(owner):
    return owner ^ 24 if owner & 32 else owner


def swap_ghosts(rows):
    groups = [list(range(8 * k, 8 * k + 8)) for k in range(DEVS // 8)]
    cube = rows.reshape(8, 32, 128)
    near = lax.all_to_all(cube, "dom", split_axis=0, concat_axis=0, axis_index_groups=groups, tiled=True)
    up = [(device_of(i), device_of((i + 8) % DEVS)) for i in range(DEVS)]
    down = [(b, a) for a, b in up]
    above = lax.ppermute(near[4:8, 16:32].reshape(64, 128), "dom", up)
    below = lax.ppermute(near[0:4, 16:32].reshape(64, 128), "dom", down)
    return near.reshape(256, 128), above, below


def local(
    modal_dofs, jacobian, face_area, cluster_id, target_slot, ghost_slots, face_neighbours,
    stiffness, star_matrix, face_minus, face_plus, solver_minus, solver_plus,
):
    owner = lax.axis_index("dom").astype(jnp.int32).reshape(1)
    target = target_slot.reshape(1, BLOCK)
    sent, tables = call(
        scatter_kernel, "scatter", [shape(CHUNK, DEVS), shape(16, SLOTS, dtype=jnp.int32)],
        [
            vmem(QUANT, MODES, BLOCK), vmem(328, BLOCK), vmem(CHUNK, DEVS), vmem(1, BLOCK, dtype=jnp.int32),
            vmem(1, BLOCK, dtype=jnp.int32), vmem(6, 1, NEIGH, dtype=jnp.int32), pltpu.SemaphoreType.DMA((7,)),
        ],
        10**8,
        (
            jnp.transpose(modal_dofs, (1, 0, 2)), jacobian, face_area, cluster_id.reshape(1, BLOCK), target,
            face_neighbours, jnp.transpose(ghost_slots, (2, 0, 1)),
        ),
        "hhhhhhh", "", FULL,
    )
    received = exchange(sent, 8)

    d_op, c_op, b_op = call(
        operator_kernel, "operators",
        [shape(2 * ROWS, k * ROWS, dtype=BF16) for k in (3, 7, 4)],
        [
            vmem(3, MODES, MODES), vmem(MODES, 4, MODES), vmem(MODES, 4, MODES),
            vmem(QUANT, 3, QUANT), vmem(QUANT, 4, QUANT), vmem(QUANT, 4, QUANT),
            vmem(14, 48, 128), vmem(128, 128), vmem(256, 128), vmem(ROWS, 7 * ROWS),
            vmem(2 * ROWS, 4 * ROWS, dtype=BF16), vmem(2 * ROWS, 7 * ROWS, dtype=BF16),
            pltpu.SemaphoreType.DMA((6,)), pltpu.SemaphoreType.DMA((2,)),
        ],
        10**9,
        (stiffness, *[jnp.transpose(a, (1, 0, 2)) for a in (face_minus, face_plus, star_matrix, solver_minus, solver_plus)]),
        "hhhhhh", "vhh", FULL - 1900 * 1024,
    )
    home = [(o, device_of(o)) for o in range(DEVS)]
    tables = lax.ppermute(tables, "dom", home)
    received, tables = lax.optimization_barrier((received, tables))
    x_scratch = [vmem(3 * ROWS, 512, dtype=BF16), vmem(3 * ROWS, 256, dtype=BF16)]
    y_scratch = [vmem(4 * ROWS, 2 * SLOTS, dtype=BF16)]
    z_scratch = [vmem(7 * ROWS, 2 * SLOTS, dtype=BF16)]
    field = shape(ROWS, SLOTS)
    halo = shape(8 * 32, 128)
    state, extras, first, later, picks, out1 = call(
        start_kernel, "start", [field, shape(8, SLOTS), field, field, shape(8, 128, dtype=jnp.int32), halo],
        [vmem(CHUNK, DEVS)] + x_scratch,
        10**9, (owner, received, tables, d_op), "s",
    )
    near, above, below = swap_ghosts(out1)
    first, _ = lax.optimization_barrier((first, near))
    partial1, faces = call(
        local_kernel, "local1", [field, shape(4, SLOTS, dtype=jnp.int32)], z_scratch, 10**9,
        (state, first, extras, c_op, tables),
    )
    middle, second, out2 = call(
        middle_kernel, "middle", [field, field, halo],
        x_scratch + y_scratch, 2 * 10**9,
        (owner, near, above, below, partial1, first, later, extras, faces, picks, d_op, b_op), "s",
    )
    near, above, below = swap_ghosts(out2)
    second, _ = lax.optimization_barrier((second, near))
    partial2 = call(
        local_terms, "local2", field, z_scratch, 10**9, (middle, second, extras, c_op)
    )
    back = call(
        final_kernel, "final", shape(CHUNK, DEVS),
        [vmem(CHUNK, DEVS)] + y_scratch, 10**9,
        (owner, near, above, below, partial2, second, extras, faces, b_op), "s",
    )
    returned = exchange(back, 8)
    result = call(
        gather_kernel, "gather", shape(QUANT, MODES, BLOCK), [vmem(CHUNK, DEVS)], 10**8, (returned, target)
    )
    return jnp.transpose(result, (1, 0, 2))


def solution(mesh):
    placed = (
        P(None, None, "dom"), P(None, "dom"), P(None, "dom"), P("dom"), P("dom"), P("dom", None, None),
        P(None, "dom"), P(), P(), P(), P(), P(), P(),
    )
    return jax.shard_map(
        local, mesh=mesh, in_specs=placed, out_specs=P(None, None, "dom"), check_vma=False
    )
```

```python
import math

import jax
import jax.numpy as jnp
from jax import lax
from jax.experimental import pallas as pl
from jax.experimental.pallas import tpu as pltpu
from jax.sharding import PartitionSpec as P

ORDER = 5
MODES = 35
QUANT = 9
FEAT = MODES * QUANT
ROWS = 320
BLOCK = 256
DEVS = 128
CAP = 3
SLOTS = 384
STRIDE = 336
CHUNK = 1024
GHOSTS = 6
NEIGH = 8
STEPS = (1, -1, 2, -2, 3, -3, 4, -4)
F32 = jnp.float32
BF16 = jnp.bfloat16
FULL = 67043328


def weights_of(lower, upper):
    return [(upper ** (k + 1) - lower ** (k + 1)) / math.factorial(k + 1) for k in range(ORDER)]


def dot(a, b):
    return jnp.dot(a, b, preferred_element_type=F32)


def split2(x):
    high = x.astype(BF16)
    return high, (x - high.astype(F32)).astype(BF16)


def split3(x):
    high = x.astype(BF16)
    rest = x - high.astype(F32)
    mid = rest.astype(BF16)
    return high, mid, (rest - mid.astype(F32)).astype(BF16)


def dot3(a, b, dims=None):
    total = None
    for part in split3(a):
        if dims is None:
            term = dot(part, b)
        else:
            term = lax.dot_general(part, b, (dims, ((), ())), preferred_element_type=F32)
        total = term if total is None else total + term
    return total


def product(op, both):
    width = both.shape[1] // 2
    wide = dot(op[0:ROWS, :], both[...])
    return wide[:, 0:width] + wide[:, width:] + dot(op[ROWS:, :], both[:, 0:width])


def put(both, at, value):
    width = both.shape[1] // 2
    high, low = split2(value)
    both[ROWS * at : ROWS * (at + 1), 0:width] = high
    both[ROWS * at : ROWS * (at + 1), width:] = low


def owner_of(device):
    return jnp.where((device & 32) > 0, device ^ 24, device)


def iota(shape, dim):
    return lax.broadcasted_iota(jnp.int32, shape, dim)


def onehot(condition):
    return jnp.where(condition, 1.0, 0.0).astype(BF16)


def pack_rows(stage, out_ref):
    for k in range(8):
        out_ref[pl.ds(k, DEVS, stride=8), :] = stage[128 * k : 128 * k + 128, :].T


def unpack_rows(recv_ref, stage):
    for k in range(8):
        stage[128 * k : 128 * k + 128, :] = recv_ref[pl.ds(k, DEVS, stride=8), :].T


def scatter_kernel(
    modal, jac, area, cluster, target, faces, listed, out, tables, cells, values, stage, kinds, places, lists, done
):
    copies = [
        pltpu.make_async_copy(modal, cells, done.at[0]),
        pltpu.make_async_copy(jac, values.at[0:3, :], done.at[1]),
        pltpu.make_async_copy(area, values.at[3:7, :], done.at[2]),
        pltpu.make_async_copy(cluster, kinds, done.at[3]),
        pltpu.make_async_copy(target, places, done.at[4]),
        pltpu.make_async_copy(faces, tables.at[0:4, :], done.at[5]),
        pltpu.make_async_copy(listed, lists, done.at[6]),
    ]
    for copy in copies:
        copy.start()
    for copy in copies:
        copy.wait()
    tables[8:16, :] = jnp.zeros((8, SLOTS), jnp.int32)
    for i in range(GHOSTS):
        tables[8 + i : 9 + i, 0:NEIGH] = lists[i]
    values[7:8, :] = 1.0 + kinds[...].astype(F32)
    values[320:328, :] = jnp.zeros((8, BLOCK), F32)
    for q in range(QUANT):
        values[8 + MODES * q : 8 + MODES * (q + 1), :] = cells[q]
    slot = owner_of(iota((DEVS, BLOCK), 0)) * CAP
    wanted = places[...]
    stage[CAP * STRIDE :, :] = jnp.zeros((CHUNK - CAP * STRIDE, DEVS), F32)
    parts = split3(values[...])
    for t in range(CAP):
        hot = onehot(slot + t == wanted)
        total = None
        for part in parts:
            term = lax.dot_general(part, hot, (((1,), (1,)), ((), ())), preferred_element_type=F32)
            total = term if total is None else total + term
        stage[STRIDE * t : STRIDE * t + 328, :] = total
        stage[STRIDE * t + 328 : STRIDE * (t + 1), :] = jnp.zeros((8, DEVS), F32)
    pack_rows(stage, out)


def gather_kernel(recv, target, out, stage):
    unpack_rows(recv, stage)
    wanted = target[...]
    slot = owner_of(iota((DEVS, BLOCK), 0)) * CAP
    total = None
    for t in range(CAP):
        part = stage[STRIDE * t + 8 : STRIDE * t + 8 + ROWS, :]
        term = dot3(part, onehot(slot + t == wanted))
        total = term if total is None else total + term
    for q in range(QUANT):
        out[q] = total[MODES * q : MODES * (q + 1), :]


def operator_kernel(
    stiffness, minus, plus, star, solver_minus, solver_plus, d_out, c_out, b_out,
    k_in, m_in, p_in, s_in, sm_in, sp_in, tiles, square, columns, stage, b_op, c_op, loads, done,
):
    copies = fetch(
        [
            (stiffness, k_in), (minus, m_in), (plus, p_in), (star, s_in),
            (solver_minus, sm_in), (solver_plus, sp_in),
        ],
        loads,
    )
    col = iota((8, 2 * ROWS), 1)
    second = jnp.where(col >= ROWS, 1, 0)
    inner = col - second * ROWS
    quant = (inner * 1873) >> 16
    mode = inner - quant * MODES
    valid = inner < FEAT
    mode_code = jnp.where(valid, second * 128 + mode, -1)[0:1]
    quant_code = jnp.where(valid, second * 16 + quant, -512)[0:1]
    row = iota((256, 2 * ROWS), 0)
    mode_hot = onehot(row == mode_code)
    tiles[...] = jnp.zeros(tiles.shape, F32)
    square[...] = jnp.zeros(square.shape, F32)
    columns[...] = jnp.zeros(columns.shape, F32)
    for copy in copies:
        copy.wait()
    for c in range(3):
        square[0:MODES, 0:MODES] = -k_in[c]
        tiles[c] = square[...].T[0:48, :]
        tiles[3 + c, 0:MODES, 0:MODES] = k_in[c]
        columns[16 * c : 16 * c + QUANT, 0:QUANT] = s_in[:, c, :]
        columns[16 * (3 + c) : 16 * (3 + c) + QUANT, 0:QUANT] = s_in[:, c, :]
    for f in range(4):
        tiles[6 + f, 0:MODES, 0:MODES] = -m_in[:, f, :]
        tiles[10 + f, 0:MODES, 0:MODES] = -p_in[:, f, :]
        columns[16 * (6 + f) : 16 * (6 + f) + QUANT, 0:QUANT] = sm_in[:, f, :]
        columns[16 * (10 + f) : 16 * (10 + f) + QUANT, 0:QUANT] = sp_in[:, f, :]
    flux = split2(jnp.concatenate([columns[0:128, :].T[0:16, :], columns[128:256, :].T[0:16, :]], axis=1))

    def family(first, count, out):
        stage[FEAT:ROWS, :] = jnp.zeros((ROWS - FEAT, stage.shape[1]), F32)
        for k in range(0, count, 2):
            width = ROWS * min(2, count - k)
            at = first + k
            after = min(at + 1, 13)
            pair = split2(jnp.concatenate([tiles[at], tiles[after]], axis=1))
            quant_hot = onehot(row == quant_code + 16 * at)
            spread = dot(pair[0], mode_hot) + dot(pair[1], mode_hot)
            scale = dot(flux[0], quant_hot) + dot(flux[1], quant_hot)
            for p in range(QUANT):
                stage[MODES * p : MODES * (p + 1), ROWS * k : ROWS * k + width] = (
                    spread[0:MODES, 0:width] * scale[p : p + 1, 0:width]
                )
        a_high, a_low = split2(stage[:, 0 : ROWS * count])
        out[0:ROWS, :] = a_high
        out[ROWS:, :] = a_low

    family(3, 7, c_op)
    copies = fetch([(c_op, c_out)], done)
    family(10, 4, b_op)
    copies += fetch([(b_op, b_out)], done, 1)
    family(0, 3, d_out)
    for copy in copies:
        copy.wait()


def order_faces(faces):
    digits = jnp.concatenate([faces >> 4, faces & 15], axis=0).astype(F32).astype(BF16)
    from_slot = iota((SLOTS, SLOTS), 0)
    to_slot = iota((SLOTS, SLOTS), 1)
    moved = dot(digits, onehot(from_slot == (to_slot & 127) * CAP + (to_slot >> 7))).astype(jnp.int32)
    return moved[0:4, :] * 16 + moved[4:8, :]


def taylor(start, extras, d_op, pieces, factor_sets):
    cuts = [(0, 256), (256, SLOTS)]
    current = [start[:, lo:hi] for lo, hi in cuts]
    sums = [[value * factors[0] for value in current] for factors in factor_sets]
    for k in range(1, ORDER):
        for i, (lo, hi) in enumerate(cuts):
            for c in range(3):
                put(pieces[i], c, current[i] * extras[c : c + 1, lo:hi])
            current[i] = product(d_op, pieces[i])
            for total, factors in zip(sums, factor_sets):
                total[i] = total[i] + current[i] * factors[k]
    return [jnp.concatenate(total, axis=1) for total in sums]


def order_picks(listed, picks):
    value = listed
    digits = jnp.concatenate([value >> 4, value & 15], axis=0).astype(F32).astype(BF16)
    spread = dot(digits, onehot(iota((128, 128), 0) == (iota((128, 128), 1) >> 3))).astype(jnp.int32)
    spread = spread[0:8, :] * 16 + spread[8:16, :]
    lane = iota((1, 128), 1)
    part = jnp.where(lane < 64, lane & 7, 8)

    def choose(*moves):
        line = jnp.full((1, 128), -1, jnp.int32)
        for ghost, spot in moves:
            line = jnp.where(part == spot, spread[ghost : ghost + 1, :], line)
        return line

    picks[...] = jnp.full(picks.shape, -1, jnp.int32)
    picks[0:1, :] = choose(*[(i, i) for i in range(GHOSTS)])
    picks[1:2, :] = choose((0, 6), (2, 7))
    picks[2:3, :] = choose((1, 6), (3, 7))
    picks[3:4, :] = choose((4, 6))
    picks[4:5, :] = choose((5, 6))


def send_ghosts(value, picks, owner, out):
    out[...] = jnp.zeros(out.shape, F32)
    slot = iota((SLOTS, 128), 0)
    slot = (slot & 127) * CAP + (slot >> 7)
    base = onehot(slot == picks[0:1, :])
    rest = jnp.concatenate([onehot(slot == picks[k : k + 1, :]) for k in range(1, 5)], axis=1)
    main = dot3(value[0:256, :], base)
    tail = dot3(value[256:320, :], rest)
    first = (main[0:128, :] + jnp.concatenate([tail[:, 0:128], tail[:, 128:256]], axis=0)).T
    second = (main[128:256, :] + jnp.concatenate([tail[:, 256:384], tail[:, 384:512]], axis=0)).T
    spot = owner & 7
    for b, step in enumerate(STEPS):
        goal = spot + step
        outside = jnp.where((goal < 0) | (goal > 7), 16, 0)
        place = ((goal + 8) & 7) * 32 + outside
        out[pl.ds(pl.multiple_of(place, 16), 8), :] = first[8 * b : 8 * b + 8, :]
        out[pl.ds(pl.multiple_of(place + 8, 8), 8), :] = second[8 * b : 8 * b + 8, :]


def read_ghosts(near, far, owner):
    firsts, seconds = [], []
    spot = owner & 7
    for step in STEPS:
        origin = spot - step
        inside = (origin >= 0) & (origin <= 7)
        place = pl.multiple_of(((origin + 8) & 7) * 32, 32)
        other = pl.multiple_of((origin & 3) * 16, 16)
        firsts.append(jnp.where(inside, near[pl.ds(place, 8), :], far[pl.ds(other, 8), :]))
        seconds.append(jnp.where(inside, near[pl.ds(place + 8, 8), :], far[pl.ds(other + 8, 8), :]))
    blank = jnp.zeros((64, 128), F32)
    first = jnp.concatenate(firsts + [blank], axis=0).T
    second = jnp.concatenate(seconds + [blank], axis=0).T
    row = iota((128, 128), 0)
    col = iota((128, 128), 1)
    part = col & 7
    group = col - part
    halves = [first[0:64, :], first[64:128, :], second[0:64, :], second[64:128, :]]
    places = [((0, 6), (2, 7)), ((1, 6), (3, 7)), ((4, 6),), ((5, 6),)]
    tail = None
    for half, moves in zip(halves, places):
        hit = None
        for ghost, spot in moves:
            one = (part == ghost) & (row == group + spot)
            hit = one if hit is None else hit | one
        term = dot3(half, onehot(hit))
        tail = term if tail is None else tail + term
    return jnp.concatenate([first, second, tail], axis=0)


def remote_flux(value, ghosts, extras, faces, b_op, both):
    high, low = split2(jnp.concatenate([value, ghosts], axis=1))
    row = iota((512, 128), 0)
    beyond = row - SLOTS
    local = (row & 127) * CAP + (row >> 7)
    spot = beyond & 7
    ghost = jnp.where((spot < GHOSTS) & (beyond < 64), SLOTS + (beyond >> 3) * GHOSTS + spot, -1)
    code = jnp.where(row < SLOTS, local, ghost)
    for f in range(4):
        hot = jnp.concatenate(
            [onehot(code == faces[f : f + 1, 128 * k : 128 * (k + 1)]) for k in range(3)], axis=1
        )
        picked = (dot(high, hot) + dot(low, hot)) * extras[3 + f : 4 + f, :]
        put(both, f, picked)
    return product(b_op, both)


def fetch(pairs, done, base=0):
    copies = [pltpu.make_async_copy(src, dst, done.at[base + k]) for k, (src, dst) in enumerate(pairs)]
    for copy in copies:
        copy.start()
    return copies


def occupied(extras):
    return jnp.where(extras[7:8, :] > 0.5, 1.0, 0.0)


def unpack_kernel(recv, tables, state, extras, picks, stage):
    order_picks(tables[8:16, 0:128], picks)
    unpack_rows(recv, stage)
    for t in range(CAP):
        extras[:, 128 * t : 128 * (t + 1)] = stage[STRIDE * t : STRIDE * t + 8, :]
        state[:, 128 * t : 128 * (t + 1)] = stage[STRIDE * t + 8 : STRIDE * t + 8 + ROWS, :]


def start_kernel(owner, state, extras, picks, d_op, first, later, ghosts, one_piece, other_piece):
    one, two = taylor(
        state[...], extras, d_op, (one_piece, other_piece), [weights_of(0.0, 1.0), weights_of(1.0, 2.0)]
    )
    first[...] = one
    later[...] = two
    send_ghosts(first, picks, owner[0], ghosts)


def local_kernel(state, value, extras, c_op, faces, out, order, both):
    order[...] = order_faces(faces[0:4, :])
    local_terms(state, value, extras, c_op, out, both)


def local_terms(state, value, extras, c_op, out, both):
    for k in range(7):
        put(both, k, value[...] * extras[k : k + 1, :])
    change = product(c_op, both)
    out[...] = state[...] + occupied(extras) * change


def middle_kernel(
    owner, near, far, partial, first, later, extras, faces, picks, d_op, b_op,
    middle, second, ghosts, one_piece, other_piece, wide,
):
    table = read_ghosts(near, far, owner[0])
    flux = remote_flux(first[...], table, extras, faces, b_op, wide)
    middle[...] = partial[...] + occupied(extras) * flux
    (fresh,) = taylor(middle[...], extras, d_op, (one_piece, other_piece), [weights_of(0.0, 1.0)])
    second[...] = jnp.where(extras[7:8, :] > 1.5, later[...], fresh)
    send_ghosts(second, picks, owner[0], ghosts)


def final_kernel(
    owner, near, far, partial, second, extras, faces, b_op, out, stage, wide
):
    table = read_ghosts(near, far, owner[0])
    flux = remote_flux(second[...], table, extras, faces, b_op, wide)
    final = partial[...] + occupied(extras) * flux
    stage[...] = jnp.zeros((CHUNK, DEVS), F32)
    for t in range(CAP):
        stage[STRIDE * t + 8 : STRIDE * t + 8 + ROWS, :] = final[:, 128 * t : 128 * (t + 1)]
    pack_rows(stage, out)


def shape(*dims, dtype=F32):
    return jax.ShapeDtypeStruct(dims, dtype)


def call(kernel, name, outs, scratch, flops, operands, spaces="", out_spaces="", limit=16 * 1024 * 1024):
    kinds = {"s": pltpu.SMEM, "v": pltpu.VMEM, "h": pltpu.HBM}
    spaces = spaces.ljust(len(operands), "v")
    flat = jax.tree.leaves(outs)
    out_specs = [pl.BlockSpec(memory_space=kinds[k]) for k in out_spaces.ljust(len(flat), "v")]
    moved = sum(math.prod(o.shape) * 4 for o in operands)
    return pl.pallas_call(
        kernel,
        name=name,
        out_shape=outs,
        in_specs=[pl.BlockSpec(memory_space=kinds[k]) for k in spaces],
        out_specs=out_specs if isinstance(outs, list) else out_specs[0],
        scratch_shapes=scratch,
        cost_estimate=pl.CostEstimate(flops=flops, bytes_accessed=moved, transcendentals=0),
        compiler_params=pltpu.CompilerParams(vmem_limit_bytes=limit),
    )(*operands)


def vmem(*dims, dtype=F32):
    return pltpu.VMEM(dims, dtype)


def exchange(rows, per):
    cube = rows.reshape(DEVS, per, 128)
    return lax.all_to_all(cube, "dom", split_axis=0, concat_axis=0, tiled=True).reshape(DEVS * per, 128)


def device_of(owner):
    return owner ^ 24 if owner & 32 else owner


def swap_ghosts(rows):
    groups = [list(range(8 * k, 8 * k + 8)) for k in range(DEVS // 8)]
    first = jnp.where((lax.axis_index("dom") & 4) == 0, 4, 0).astype(jnp.uint32)
    rows, first = lax.optimization_barrier((rows, first))
    cube = rows.reshape(8, 32, 128)
    near = lax.all_to_all(cube, "dom", split_axis=0, concat_axis=0, axis_index_groups=groups, tiled=True)
    relay = lax.dynamic_slice(near, (first, jnp.uint32(16), jnp.uint32(0)), (4, 16, 128)).reshape(64, 128)
    pairs = [(device_of(o), device_of((o + (8 if o & 4 == 0 else -8)) % DEVS)) for o in range(DEVS)]
    return near.reshape(256, 128), lax.ppermute(relay, "dom", pairs)


def local(
    modal_dofs, jacobian, face_area, cluster_id, target_slot, ghost_slots, face_neighbours,
    stiffness, star_matrix, face_minus, face_plus, solver_minus, solver_plus,
):
    owner = lax.axis_index("dom").astype(jnp.int32).reshape(1)
    target = target_slot.reshape(1, BLOCK)
    sent, tables = call(
        scatter_kernel, "scatter", [shape(CHUNK, DEVS), shape(16, SLOTS, dtype=jnp.int32)],
        [
            vmem(QUANT, MODES, BLOCK), vmem(328, BLOCK), vmem(CHUNK, DEVS), vmem(1, BLOCK, dtype=jnp.int32),
            vmem(1, BLOCK, dtype=jnp.int32), vmem(6, 1, NEIGH, dtype=jnp.int32), pltpu.SemaphoreType.DMA((7,)),
        ],
        10**8,
        (
            jnp.transpose(modal_dofs, (1, 0, 2)), jacobian, face_area, cluster_id.reshape(1, BLOCK), target,
            face_neighbours, jnp.transpose(ghost_slots, (2, 0, 1)),
        ),
        "hhhhhhh", "", FULL,
    )
    received = exchange(sent, 8)

    d_op, c_op, b_op = call(
        operator_kernel, "operators",
        [shape(2 * ROWS, k * ROWS, dtype=BF16) for k in (3, 7, 4)],
        [
            vmem(3, MODES, MODES), vmem(MODES, 4, MODES), vmem(MODES, 4, MODES),
            vmem(QUANT, 3, QUANT), vmem(QUANT, 4, QUANT), vmem(QUANT, 4, QUANT),
            vmem(14, 48, 128), vmem(128, 128), vmem(256, 128), vmem(ROWS, 7 * ROWS),
            vmem(2 * ROWS, 4 * ROWS, dtype=BF16), vmem(2 * ROWS, 7 * ROWS, dtype=BF16),
            pltpu.SemaphoreType.DMA((6,)), pltpu.SemaphoreType.DMA((2,)),
        ],
        10**9,
        (stiffness, *[jnp.transpose(a, (1, 0, 2)) for a in (face_minus, face_plus, star_matrix, solver_minus, solver_plus)]),
        "hhhhhh", "vhh", FULL - 1900 * 1024,
    )
    home = [(o, device_of(o)) for o in range(DEVS)]
    tables = lax.ppermute(tables, "dom", home)
    received, tables = lax.optimization_barrier((received, tables))
    x_scratch = [vmem(3 * ROWS, 512, dtype=BF16), vmem(3 * ROWS, 256, dtype=BF16)]
    y_scratch = [vmem(4 * ROWS, 2 * SLOTS, dtype=BF16)]
    z_scratch = [vmem(7 * ROWS, 2 * SLOTS, dtype=BF16)]
    field = shape(ROWS, SLOTS)
    halo = shape(8 * 32, 128)
    state, extras, picks = call(
        unpack_kernel, "unpack", [field, shape(8, SLOTS), shape(8, 128, dtype=jnp.int32)],
        [vmem(CHUNK, DEVS)], 10**8, (received, tables),
    )
    first, later, out1 = call(
        start_kernel, "start", [field, field, halo], x_scratch, 10**9, (owner, state, extras, picks, d_op), "s",
    )
    near, far = swap_ghosts(out1)
    first, _ = lax.optimization_barrier((first, near))
    partial1, faces = call(
        local_kernel, "local1", [field, shape(4, SLOTS, dtype=jnp.int32)], z_scratch, 10**9,
        (state, first, extras, c_op, tables),
    )
    middle, second, out2 = call(
        middle_kernel, "middle", [field, field, halo],
        x_scratch + y_scratch, 2 * 10**9,
        (owner, near, far, partial1, first, later, extras, faces, picks, d_op, b_op), "s",
    )
    near, far = swap_ghosts(out2)
    second, _ = lax.optimization_barrier((second, near))
    partial2 = call(
        local_terms, "local2", field, z_scratch, 10**9, (middle, second, extras, c_op)
    )
    back = call(
        final_kernel, "final", shape(CHUNK, DEVS),
        [vmem(CHUNK, DEVS)] + y_scratch, 10**9,
        (owner, near, far, partial2, second, extras, faces, b_op), "s",
    )
    returned = exchange(back, 8)
    result = call(
        gather_kernel, "gather", shape(QUANT, MODES, BLOCK), [vmem(CHUNK, DEVS)], 10**8, (returned, target)
    )
    return jnp.transpose(result, (1, 0, 2))


def solution(mesh):
    placed = (
        P(None, None, "dom"), P(None, "dom"), P(None, "dom"), P("dom"), P("dom"), P("dom", None, None),
        P(None, "dom"), P(), P(), P(), P(), P(), P(),
    )
    return jax.shard_map(
        local, mesh=mesh, in_specs=placed, out_specs=P(None, None, "dom"), check_vma=False
    )
```

```python
import math

import jax
import jax.numpy as jnp
from jax import lax
from jax.experimental import pallas as pl
from jax.experimental.pallas import tpu as pltpu
from jax.sharding import PartitionSpec as P

ORDER = 5
MODES = 35
QUANT = 9
FEAT = MODES * QUANT
ROWS = 320
BLOCK = 256
DEVS = 128
CAP = 3
SLOTS = 384
STRIDE = 336
CHUNK = 1024
GHOSTS = 6
NEIGH = 8
STEPS = (1, -1, 2, -2, 3, -3, 4, -4)
F32 = jnp.float32
BF16 = jnp.bfloat16
FULL = 67043328


def weights_of(lower, upper):
    return [(upper ** (k + 1) - lower ** (k + 1)) / math.factorial(k + 1) for k in range(ORDER)]


def dot(a, b):
    return jnp.dot(a, b, preferred_element_type=F32)


def split2(x):
    high = x.astype(BF16)
    return high, (x - high.astype(F32)).astype(BF16)


def split3(x):
    high = x.astype(BF16)
    rest = x - high.astype(F32)
    mid = rest.astype(BF16)
    return high, mid, (rest - mid.astype(F32)).astype(BF16)


def dot3(a, b, dims=None):
    total = None
    for part in split3(a):
        if dims is None:
            term = dot(part, b)
        else:
            term = lax.dot_general(part, b, (dims, ((), ())), preferred_element_type=F32)
        total = term if total is None else total + term
    return total


def product(op, both):
    depth, width = both.shape[0], both.shape[1] // 2
    wide = dot(op[0:ROWS, 0:depth], both[...])
    return wide[:, 0:width] + wide[:, width:] + dot(op[ROWS:, 0:depth], both[:, 0:width])


def put(both, at, value):
    width = both.shape[1] // 2
    high, low = split2(value)
    both[ROWS * at : ROWS * (at + 1), 0:width] = high
    both[ROWS * at : ROWS * (at + 1), width:] = low


PATH = (0, 1, 2, 3, 7, 11, 15, 14, 10, 6, 5, 9, 13, 12, 8, 4)


def owner_of(device):
    group = device >> 3
    place = jnp.zeros_like(group)
    for k, g in enumerate(PATH):
        place = jnp.where(group == g, k, place)
    return place * 8 + (device & 7)


def device_of(owner):
    return PATH[owner // 8] * 8 + owner % 8


def iota(shape, dim):
    return lax.broadcasted_iota(jnp.int32, shape, dim)


def onehot(condition):
    return jnp.where(condition, 1.0, 0.0).astype(BF16)


def pack_rows(stage, out_ref):
    for k in range(8):
        out_ref[pl.ds(k, DEVS, stride=8), :] = stage[128 * k : 128 * k + 128, :].T


def unpack_rows(recv_ref, stage):
    for k in range(8):
        stage[128 * k : 128 * k + 128, :] = recv_ref[pl.ds(k, DEVS, stride=8), :].T


def scatter_kernel(
    modal, jac, area, cluster, target, faces, listed, out, tables, cells, values, stage, kinds, places, lists, done
):
    copies = [
        pltpu.make_async_copy(modal, cells, done.at[0]),
        pltpu.make_async_copy(jac, values.at[0:3, :], done.at[1]),
        pltpu.make_async_copy(area, values.at[3:7, :], done.at[2]),
        pltpu.make_async_copy(cluster, kinds, done.at[3]),
        pltpu.make_async_copy(target, places, done.at[4]),
        pltpu.make_async_copy(faces, tables.at[0:4, :], done.at[5]),
        pltpu.make_async_copy(listed, lists, done.at[6]),
    ]
    for copy in copies:
        copy.start()
    for copy in copies:
        copy.wait()
    tables[8:16, :] = jnp.zeros((8, SLOTS), jnp.int32)
    for i in range(GHOSTS):
        tables[8 + i : 9 + i, 0:NEIGH] = lists[i]
    values[7:8, :] = 1.0 + kinds[...].astype(F32)
    values[320:328, :] = jnp.zeros((8, BLOCK), F32)
    for q in range(QUANT):
        values[8 + MODES * q : 8 + MODES * (q + 1), :] = cells[q]
    half = owner_of(iota((DEVS, DEVS), 0)) * CAP
    slot = jnp.concatenate([half, half], axis=1)
    wanted = places[...]
    stage[CAP * STRIDE :, :] = jnp.zeros((CHUNK - CAP * STRIDE, DEVS), F32)
    parts = split3(values[...])
    for t in range(CAP):
        hot = onehot(slot + t == wanted)
        total = None
        for part in parts:
            term = lax.dot_general(part, hot, (((1,), (1,)), ((), ())), preferred_element_type=F32)
            total = term if total is None else total + term
        stage[STRIDE * t : STRIDE * t + 328, :] = total
        stage[STRIDE * t + 328 : STRIDE * (t + 1), :] = jnp.zeros((8, DEVS), F32)
    pack_rows(stage, out)


def gather_kernel(recv, target, out, stage):
    unpack_rows(recv, stage)
    wanted = target[...]
    half = owner_of(iota((DEVS, DEVS), 0)) * CAP
    slot = jnp.concatenate([half, half], axis=1)
    total = None
    for t in range(CAP):
        part = stage[STRIDE * t + 8 : STRIDE * t + 8 + ROWS, :]
        term = dot3(part, onehot(slot + t == wanted))
        total = term if total is None else total + term
    for q in range(QUANT):
        out[q] = total[MODES * q : MODES * (q + 1), :]


def pair_codes():
    col = iota((8, 2 * ROWS), 1)
    second = jnp.where(col >= ROWS, 1, 0)
    inner = col - second * ROWS
    quant = (inner * 1873) >> 16
    mode = inner - quant * MODES
    valid = inner < FEAT
    mode_code = jnp.where(valid, second * 128 + mode, -1)[0:1]
    quant_code = jnp.where(valid, second * 16 + quant, -512)[0:1]
    row = iota((256, 2 * ROWS), 0)
    return row, onehot(row == mode_code), quant_code


def expand_pairs(first, last, count, tiles, columns, codes, stage, op, ready):
    row, mode_hot, quant_code = codes
    flux = split2(jnp.concatenate([columns[0:128, :].T[0:16, :], columns[128:256, :].T[0:16, :]], axis=1))
    for k in range(0, count, 2):
        width = ROWS * min(2, count - k)
        at = first + k
        pair = split2(jnp.concatenate([tiles[at], tiles[min(at + 1, last)]], axis=1))
        quant_hot = onehot(row == quant_code + 16 * at)
        spread = dot(pair[0], mode_hot) + dot(pair[1], mode_hot)
        scale = dot(flux[0], quant_hot) + dot(flux[1], quant_hot)
        for p in range(QUANT):
            stage[MODES * p : MODES * (p + 1), 0:width] = spread[0:MODES, 0:width] * scale[p : p + 1, 0:width]
        high, low = split2(stage[:, 0:width])
        op[0:ROWS, ROWS * k : ROWS * k + width] = high
        op[ROWS:, ROWS * k : ROWS * k + width] = low
        ready(slice(ROWS * k, ROWS * k + -(-width // 128) * 128))


def taylor_operator_kernel(stiffness, star, op, tiles, square, columns, stage):
    tiles[...] = jnp.zeros(tiles.shape, F32)
    square[...] = jnp.zeros(square.shape, F32)
    columns[...] = jnp.zeros(columns.shape, F32)
    stage[FEAT:ROWS, :] = jnp.zeros((ROWS - FEAT, stage.shape[1]), F32)
    for c in range(3):
        square[0:MODES, 0:MODES] = -stiffness[c]
        tiles[c] = square[...].T[0:48, :]
        columns[16 * c : 16 * c + QUANT, 0:QUANT] = star[:, c, :]
    expand_pairs(0, 2, 3, tiles, columns, pair_codes(), stage, op, lambda lanes: None)


def operator_kernel(
    stiffness, minus, plus, star, solver_minus, solver_plus, c_out, b_out,
    k_in, m_in, p_in, s_in, sm_in, sp_in, tiles, columns, stage, c_op, b_op, loads, done,
):
    copies = fetch(
        [
            (stiffness, k_in), (minus, m_in), (plus, p_in), (star, s_in),
            (solver_minus, sm_in), (solver_plus, sp_in),
        ],
        loads,
    )
    codes = pair_codes()
    tiles[...] = jnp.zeros(tiles.shape, F32)
    columns[...] = jnp.zeros(columns.shape, F32)
    stage[FEAT:ROWS, :] = jnp.zeros((ROWS - FEAT, stage.shape[1]), F32)
    for copy in copies:
        copy.wait()
    for c in range(3):
        tiles[c, 0:MODES, 0:MODES] = k_in[c]
        columns[16 * c : 16 * c + QUANT, 0:QUANT] = s_in[:, c, :]
    for f in range(4):
        tiles[3 + f, 0:MODES, 0:MODES] = -m_in[:, f, :]
        tiles[7 + f, 0:MODES, 0:MODES] = -p_in[:, f, :]
        columns[16 * (3 + f) : 16 * (3 + f) + QUANT, 0:QUANT] = sm_in[:, f, :]
        columns[16 * (7 + f) : 16 * (7 + f) + QUANT, 0:QUANT] = sp_in[:, f, :]
    sent = []

    def leave(op, out):
        return lambda lanes: sent.extend(fetch([(op.at[:, lanes], out.at[:, lanes])], done, len(sent)))

    expand_pairs(0, 10, 7, tiles, columns, codes, stage, c_op, leave(c_op, c_out))
    expand_pairs(7, 10, 4, tiles, columns, codes, stage, b_op, leave(b_op, b_out))
    for copy in sent:
        copy.wait()


def order_faces(faces):
    digits = jnp.concatenate([faces >> 4, faces & 15], axis=0).astype(F32).astype(BF16)
    from_slot = iota((SLOTS, SLOTS), 0)
    to_slot = iota((SLOTS, SLOTS), 1)
    moved = dot(digits, onehot(from_slot == (to_slot & 127) * CAP + (to_slot >> 7))).astype(jnp.int32)
    return moved[0:4, :] * 16 + moved[4:8, :]


def taylor(start, extras, d_op, pieces, factor_sets):
    cuts = [(0, 256), (256, SLOTS)]
    current = [start[:, lo:hi] for lo, hi in cuts]
    sums = [[value * factors[0] for value in current] for factors in factor_sets]
    for k in range(1, ORDER):
        for i, (lo, hi) in enumerate(cuts):
            for c in range(3):
                put(pieces[i], c, current[i] * extras[c : c + 1, lo:hi])
            current[i] = product(d_op, pieces[i])
            for total, factors in zip(sums, factor_sets):
                total[i] = total[i] + current[i] * factors[k]
    return [jnp.concatenate(total, axis=1) for total in sums]


def order_picks(listed, picks):
    value = listed
    digits = jnp.concatenate([value >> 4, value & 15], axis=0).astype(F32).astype(BF16)
    spread = dot(digits, onehot(iota((128, 128), 0) == (iota((128, 128), 1) >> 3))).astype(jnp.int32)
    spread = spread[0:8, :] * 16 + spread[8:16, :]
    lane = iota((1, 128), 1)
    part = jnp.where(lane < 64, lane & 7, 8)

    def choose(*moves):
        line = jnp.full((1, 128), -1, jnp.int32)
        for ghost, spot in moves:
            line = jnp.where(part == spot, spread[ghost : ghost + 1, :], line)
        return line

    picks[...] = jnp.full(picks.shape, -1, jnp.int32)
    picks[0:1, :] = choose(*[(i, i) for i in range(GHOSTS)])
    picks[1:2, :] = choose((0, 6), (2, 7))
    picks[2:3, :] = choose((1, 6), (3, 7))
    picks[3:4, :] = choose((4, 6))
    picks[4:5, :] = choose((5, 6))


def send_ghosts(value, picks, owner, out):
    out[...] = jnp.zeros(out.shape, F32)
    slot = iota((SLOTS, 128), 0)
    slot = (slot & 127) * CAP + (slot >> 7)
    base = onehot(slot == picks[0:1, :])
    rest = jnp.concatenate([onehot(slot == picks[k : k + 1, :]) for k in range(1, 5)], axis=1)
    main = dot3(value[0:256, :], base)
    tail = dot3(value[256:320, :], rest)
    first = (main[0:128, :] + jnp.concatenate([tail[:, 0:128], tail[:, 128:256]], axis=0)).T
    second = (main[128:256, :] + jnp.concatenate([tail[:, 256:384], tail[:, 384:512]], axis=0)).T
    spot = owner & 7
    for b, step in enumerate(STEPS):
        goal = spot + step
        outside = jnp.where((goal < 0) | (goal > 7), 16, 0)
        place = ((goal + 8) & 7) * 32 + outside
        out[pl.ds(pl.multiple_of(place, 16), 8), :] = first[8 * b : 8 * b + 8, :]
        out[pl.ds(pl.multiple_of(place + 8, 8), 8), :] = second[8 * b : 8 * b + 8, :]


def read_ghosts(near, far, owner):
    firsts, seconds = [], []
    spot = owner & 7
    for step in STEPS:
        origin = spot - step
        inside = (origin >= 0) & (origin <= 7)
        place = pl.multiple_of(((origin + 8) & 7) * 32, 32)
        other = pl.multiple_of((origin & 3) * 16, 16)
        firsts.append(jnp.where(inside, near[pl.ds(place, 8), :], far[pl.ds(other, 8), :]))
        seconds.append(jnp.where(inside, near[pl.ds(place + 8, 8), :], far[pl.ds(other + 8, 8), :]))
    blank = jnp.zeros((64, 128), F32)
    first = jnp.concatenate(firsts + [blank], axis=0).T
    second = jnp.concatenate(seconds + [blank], axis=0).T
    row = iota((128, 128), 0)
    col = iota((128, 128), 1)
    part = col & 7
    group = col - part
    halves = [first[0:64, :], first[64:128, :], second[0:64, :], second[64:128, :]]
    places = [((0, 6), (2, 7)), ((1, 6), (3, 7)), ((4, 6),), ((5, 6),)]
    tail = None
    for half, moves in zip(halves, places):
        hit = None
        for ghost, spot in moves:
            one = (part == ghost) & (row == group + spot)
            hit = one if hit is None else hit | one
        term = dot3(half, onehot(hit))
        tail = term if tail is None else tail + term
    return jnp.concatenate([first, second, tail], axis=0)


def remote_flux(value, ghosts, extras, faces, b_op, both):
    high, low = split2(jnp.concatenate([value, ghosts], axis=1))
    row = iota((512, 128), 0)
    beyond = row - SLOTS
    local = (row & 127) * CAP + (row >> 7)
    spot = beyond & 7
    ghost = jnp.where((spot < GHOSTS) & (beyond < 64), SLOTS + (beyond >> 3) * GHOSTS + spot, -1)
    code = jnp.where(row < SLOTS, local, ghost)
    for f in range(4):
        hot = jnp.concatenate(
            [onehot(code == faces[f : f + 1, 128 * k : 128 * (k + 1)]) for k in range(3)], axis=1
        )
        picked = (dot(high, hot) + dot(low, hot)) * extras[3 + f : 4 + f, :]
        put(both, f, picked)
    return product(b_op, both)


def fetch(pairs, done, base=0):
    copies = [pltpu.make_async_copy(src, dst, done.at[base + k]) for k, (src, dst) in enumerate(pairs)]
    for copy in copies:
        copy.start()
    return copies


def occupied(extras):
    return jnp.where(extras[7:8, :] > 0.5, 1.0, 0.0)


def unpack_kernel(recv, tables, state, extras, picks, stage):
    order_picks(tables[8:16, 0:128], picks)
    unpack_rows(recv, stage)
    for t in range(CAP):
        extras[:, 128 * t : 128 * (t + 1)] = stage[STRIDE * t : STRIDE * t + 8, :]
        state[:, 128 * t : 128 * (t + 1)] = stage[STRIDE * t + 8 : STRIDE * t + 8 + ROWS, :]


def start_kernel(owner, state, extras, picks, d_op, first, later, ghosts, one_piece, other_piece):
    one, two = taylor(
        state[...], extras, d_op, (one_piece, other_piece), [weights_of(0.0, 1.0), weights_of(1.0, 2.0)]
    )
    first[...] = one
    later[...] = two
    send_ghosts(first, picks, owner[0], ghosts)


def local_kernel(state, value, extras, c_op, faces, out, order, both):
    order[...] = order_faces(faces[0:4, :])
    local_terms(state, value, extras, c_op, out, both)


def local_terms(state, value, extras, c_op, out, both):
    for k in range(7):
        put(both, k, value[...] * extras[k : k + 1, :])
    change = product(c_op, both)
    out[...] = state[...] + occupied(extras) * change


def middle_kernel(
    owner, near, far, partial, first, later, extras, faces, picks, d_op, b_op,
    middle, second, ghosts, one_piece, other_piece, wide,
):
    table = read_ghosts(near, far, owner[0])
    flux = remote_flux(first[...], table, extras, faces, b_op, wide)
    middle[...] = partial[...] + occupied(extras) * flux
    (fresh,) = taylor(middle[...], extras, d_op, (one_piece, other_piece), [weights_of(0.0, 1.0)])
    second[...] = jnp.where(extras[7:8, :] > 1.5, later[...], fresh)
    send_ghosts(second, picks, owner[0], ghosts)


def final_kernel(
    owner, near, far, partial, second, extras, faces, b_op, out, stage, wide
):
    table = read_ghosts(near, far, owner[0])
    flux = remote_flux(second[...], table, extras, faces, b_op, wide)
    final = partial[...] + occupied(extras) * flux
    stage[...] = jnp.zeros((CHUNK, DEVS), F32)
    for t in range(CAP):
        stage[STRIDE * t + 8 : STRIDE * t + 8 + ROWS, :] = final[:, 128 * t : 128 * (t + 1)]
    pack_rows(stage, out)


def shape(*dims, dtype=F32):
    return jax.ShapeDtypeStruct(dims, dtype)


def call(kernel, name, outs, scratch, flops, operands, spaces="", out_spaces="", limit=16 * 1024 * 1024):
    kinds = {"s": pltpu.SMEM, "v": pltpu.VMEM, "h": pltpu.HBM}
    spaces = spaces.ljust(len(operands), "v")
    flat = jax.tree.leaves(outs)
    out_specs = [pl.BlockSpec(memory_space=kinds[k]) for k in out_spaces.ljust(len(flat), "v")]
    moved = sum(math.prod(o.shape) * 4 for o in operands)
    return pl.pallas_call(
        kernel,
        name=name,
        out_shape=outs,
        in_specs=[pl.BlockSpec(memory_space=kinds[k]) for k in spaces],
        out_specs=out_specs if isinstance(outs, list) else out_specs[0],
        scratch_shapes=scratch,
        cost_estimate=pl.CostEstimate(flops=flops, bytes_accessed=moved, transcendentals=0),
        compiler_params=pltpu.CompilerParams(vmem_limit_bytes=limit),
    )(*operands)


def vmem(*dims, dtype=F32):
    return pltpu.VMEM(dims, dtype)


def exchange(rows, per):
    cube = rows.reshape(DEVS, per, 128)
    return lax.all_to_all(cube, "dom", split_axis=0, concat_axis=0, tiled=True).reshape(DEVS * per, 128)


def swap_ghosts(rows):
    groups = [list(range(8 * k, 8 * k + 8)) for k in range(DEVS // 8)]
    first = jnp.where((lax.axis_index("dom") & 4) == 0, 4, 0).astype(jnp.uint32)
    rows, first = lax.optimization_barrier((rows, first))
    cube = rows.reshape(8, 32, 128)
    near = lax.all_to_all(cube, "dom", split_axis=0, concat_axis=0, axis_index_groups=groups, tiled=True)
    relay = lax.dynamic_slice(near, (first, jnp.uint32(16), jnp.uint32(0)), (4, 16, 128)).reshape(64, 128)
    pairs = [(device_of(o), device_of((o + (8 if o & 4 == 0 else -8)) % DEVS)) for o in range(DEVS)]
    return near.reshape(256, 128), lax.ppermute(relay, "dom", pairs)


def local(
    modal_dofs, jacobian, face_area, cluster_id, target_slot, ghost_slots, face_neighbours,
    stiffness, star_matrix, face_minus, face_plus, solver_minus, solver_plus,
):
    owner = lax.axis_index("dom").astype(jnp.int32).reshape(1)
    target = target_slot.reshape(1, BLOCK)
    sent, tables = call(
        scatter_kernel, "scatter", [shape(CHUNK, DEVS), shape(16, SLOTS, dtype=jnp.int32)],
        [
            vmem(QUANT, MODES, BLOCK), vmem(328, BLOCK), vmem(CHUNK, DEVS), vmem(1, BLOCK, dtype=jnp.int32),
            vmem(1, BLOCK, dtype=jnp.int32), vmem(6, 1, NEIGH, dtype=jnp.int32), pltpu.SemaphoreType.DMA((7,)),
        ],
        10**8,
        (
            jnp.transpose(modal_dofs, (1, 0, 2)), jacobian, face_area, cluster_id.reshape(1, BLOCK), target,
            face_neighbours, jnp.transpose(ghost_slots, (2, 0, 1)),
        ),
        "hhhhhhh", "", FULL,
    )
    received = exchange(sent, 8)

    star, minus, plus, solve_minus, solve_plus = [
        jnp.transpose(a, (1, 0, 2)) for a in (star_matrix, face_minus, face_plus, solver_minus, solver_plus)
    ]
    c_op, b_op = call(
        operator_kernel, "operators",
        [shape(2 * ROWS, w, dtype=BF16) for w in (2304, 1280)],
        [
            vmem(3, MODES, MODES), vmem(MODES, 4, MODES), vmem(MODES, 4, MODES),
            vmem(QUANT, 3, QUANT), vmem(QUANT, 4, QUANT), vmem(QUANT, 4, QUANT),
            vmem(11, 48, 128), vmem(256, 128), vmem(ROWS, 2 * ROWS), vmem(2 * ROWS, 2304, dtype=BF16),
            vmem(2 * ROWS, 1280, dtype=BF16), pltpu.SemaphoreType.DMA((6,)), pltpu.SemaphoreType.DMA((6,)),
        ],
        10**9, (stiffness, minus, plus, star, solve_minus, solve_plus), "hhhhhh", "hh", FULL - 1900 * 1024,
    )
    stiffness, star, _ = lax.optimization_barrier((stiffness, star, b_op))
    d_op = call(
        taylor_operator_kernel, "taylor_operators", shape(2 * ROWS, 960, dtype=BF16),
        [vmem(3, 48, 128), vmem(128, 128), vmem(256, 128), vmem(ROWS, 2 * ROWS)],
        10**9, (stiffness, star),
    )
    home = [(o, device_of(o)) for o in range(DEVS)]
    tables = lax.ppermute(tables, "dom", home)
    received, tables = lax.optimization_barrier((received, tables))
    x_scratch = [vmem(3 * ROWS, 512, dtype=BF16), vmem(3 * ROWS, 256, dtype=BF16)]
    y_scratch = [vmem(4 * ROWS, 2 * SLOTS, dtype=BF16)]
    z_scratch = [vmem(7 * ROWS, 2 * SLOTS, dtype=BF16)]
    field = shape(ROWS, SLOTS)
    halo = shape(8 * 32, 128)
    state, extras, picks = call(
        unpack_kernel, "unpack", [field, shape(8, SLOTS), shape(8, 128, dtype=jnp.int32)],
        [vmem(CHUNK, DEVS)], 10**8, (received, tables),
    )
    first, later, out1 = call(
        start_kernel, "start", [field, field, halo], x_scratch, 10**9, (owner, state, extras, picks, d_op), "s",
    )
    near, far = swap_ghosts(out1)
    first, _ = lax.optimization_barrier((first, near))
    partial1, faces = call(
        local_kernel, "local1", [field, shape(4, SLOTS, dtype=jnp.int32)], z_scratch, 10**9,
        (state, first, extras, c_op, tables),
    )
    middle, second, out2 = call(
        middle_kernel, "middle", [field, field, halo],
        x_scratch + y_scratch, 2 * 10**9,
        (owner, near, far, partial1, first, later, extras, faces, picks, d_op, b_op), "s",
    )
    near, far = swap_ghosts(out2)
    second, _ = lax.optimization_barrier((second, near))
    partial2 = call(
        local_terms, "local2", field, z_scratch, 10**9, (middle, second, extras, c_op)
    )
    back = call(
        final_kernel, "final", shape(CHUNK, DEVS),
        [vmem(CHUNK, DEVS)] + y_scratch, 10**9,
        (owner, near, far, partial2, second, extras, faces, b_op), "s",
    )
    returned = exchange(back, 8)
    result = call(
        gather_kernel, "gather", shape(QUANT, MODES, BLOCK), [vmem(CHUNK, DEVS)], 10**8, (returned, target)
    )
    return jnp.transpose(result, (1, 0, 2))


def solution(mesh):
    placed = (
        P(None, None, "dom"), P(None, "dom"), P(None, "dom"), P("dom"), P("dom"), P("dom", None, None),
        P(None, "dom"), P(), P(), P(), P(), P(), P(),
    )
    return jax.shard_map(
        local, mesh=mesh, in_specs=placed, out_specs=P(None, None, "dom"), check_vma=False
    )
```

```python
import math

import jax
import jax.numpy as jnp
from jax import lax
from jax.experimental import pallas as pl
from jax.experimental.pallas import tpu as pltpu
from jax.sharding import PartitionSpec as P

ORDER = 5
MODES = 35
QUANT = 9
FEAT = MODES * QUANT
ROWS = 320
BLOCK = 256
DEVS = 128
CAP = 3
SLOTS = 384
STRIDE = 336
CHUNK = 1024
GHOSTS = 6
NEIGH = 8
STEPS = (1, -1, 2, -2, 3, -3, 4, -4)
SENT = (1, -1, 3, -3, 2, -2, 4, -4)
F32 = jnp.float32
BF16 = jnp.bfloat16
FULL = 67043328


def weights_of(lower, upper):
    return [(upper ** (k + 1) - lower ** (k + 1)) / math.factorial(k + 1) for k in range(ORDER)]


def dot(a, b):
    return jnp.dot(a, b, preferred_element_type=F32)


def split2(x):
    high = x.astype(BF16)
    return high, (x - high.astype(F32)).astype(BF16)


def split3(x):
    high = x.astype(BF16)
    rest = x - high.astype(F32)
    mid = rest.astype(BF16)
    return high, mid, (rest - mid.astype(F32)).astype(BF16)


def dot3(a, b, dims=None):
    total = None
    for part in split3(a):
        if dims is None:
            term = dot(part, b)
        else:
            term = lax.dot_general(part, b, (dims, ((), ())), preferred_element_type=F32)
        total = term if total is None else total + term
    return total


def product(op, both):
    depth, width = both.shape[0], both.shape[1] // 2
    wide = dot(op[0:ROWS, 0:depth], both[...])
    return wide[:, 0:width] + wide[:, width:] + dot(op[ROWS:, 0:depth], both[:, 0:width])


def put(both, at, value):
    width = both.shape[1] // 2
    high, low = split2(value)
    both[ROWS * at : ROWS * (at + 1), 0:width] = high
    both[ROWS * at : ROWS * (at + 1), width:] = low


PATH = (0, 1, 2, 3, 7, 11, 15, 14, 10, 6, 5, 9, 13, 12, 8, 4)


def owner_of(device):
    group = device >> 3
    place = jnp.zeros_like(group)
    for k, g in enumerate(PATH):
        place = jnp.where(group == g, k, place)
    inner = device & 7
    return place * 8 + jnp.where((place & 1) > 0, inner ^ 6, inner)


def device_of(owner):
    group = owner // 8
    return PATH[group] * 8 + (owner % 8 ^ (6 if group % 2 else 0))


def iota(shape, dim):
    return lax.broadcasted_iota(jnp.int32, shape, dim)


def onehot(condition):
    return jnp.where(condition, 1.0, 0.0).astype(BF16)


def pack_rows(stage, out_ref):
    for k in range(8):
        out_ref[pl.ds(k, DEVS, stride=8), :] = stage[128 * k : 128 * k + 128, :].T


def unpack_rows(recv_ref, stage):
    for k in range(8):
        stage[128 * k : 128 * k + 128, :] = recv_ref[pl.ds(k, DEVS, stride=8), :].T


def scatter_kernel(
    core, modal, jac, area, cluster, target, faces, listed, out, tables, cells, values, stage, kinds, places, lists, done
):
    copies = [
        pltpu.make_async_copy(modal, cells, done.at[0]),
        pltpu.make_async_copy(jac, values.at[0:3, :], done.at[1]),
        pltpu.make_async_copy(area, values.at[3:7, :], done.at[2]),
        pltpu.make_async_copy(cluster, kinds, done.at[3]),
        pltpu.make_async_copy(target, places, done.at[4]),
        pltpu.make_async_copy(faces, tables.at[0:4, :], done.at[5]),
        pltpu.make_async_copy(listed, lists, done.at[6]),
    ]
    for copy in copies:
        copy.start()
    for copy in copies:
        copy.wait()
    tables[4:8, :] = jnp.full((4, SLOTS), core[0], jnp.int32)
    tables[8:16, :] = jnp.zeros((8, SLOTS), jnp.int32)
    for i in range(GHOSTS):
        tables[8 + i : 9 + i, 0:NEIGH] = lists[i]
    values[7:8, :] = 1.0 + kinds[...].astype(F32)
    values[320:328, :] = jnp.zeros((8, BLOCK), F32)
    for q in range(QUANT):
        values[8 + MODES * q : 8 + MODES * (q + 1), :] = cells[q]
    half = owner_of(iota((DEVS, DEVS), 0)) * CAP
    slot = jnp.concatenate([half, half], axis=1)
    wanted = places[...]
    stage[CAP * STRIDE :, :] = jnp.zeros((CHUNK - CAP * STRIDE, DEVS), F32)
    parts = split3(values[...])
    for t in range(CAP):
        hot = onehot(slot + t == wanted)
        total = None
        for part in parts:
            term = lax.dot_general(part, hot, (((1,), (1,)), ((), ())), preferred_element_type=F32)
            total = term if total is None else total + term
        stage[STRIDE * t : STRIDE * t + 328, :] = total
        stage[STRIDE * t + 328 : STRIDE * (t + 1), :] = jnp.zeros((8, DEVS), F32)
    pack_rows(stage, out)


def gather_kernel(recv, target, out, stage):
    unpack_rows(recv, stage)
    wanted = target[...]
    half = owner_of(iota((DEVS, DEVS), 0)) * CAP
    slot = jnp.concatenate([half, half], axis=1)
    total = None
    for t in range(CAP):
        part = stage[STRIDE * t + 8 : STRIDE * t + 8 + ROWS, :]
        term = dot3(part, onehot(slot + t == wanted))
        total = term if total is None else total + term
    for q in range(QUANT):
        out[q] = total[MODES * q : MODES * (q + 1), :]


def pair_codes():
    col = iota((8, 2 * ROWS), 1)
    second = jnp.where(col >= ROWS, 1, 0)
    inner = col - second * ROWS
    quant = (inner * 1873) >> 16
    mode = inner - quant * MODES
    valid = inner < FEAT
    mode_code = jnp.where(valid, second * 128 + mode, -1)[0:1]
    quant_code = jnp.where(valid, second * 16 + quant, -512)[0:1]
    row = iota((256, 2 * ROWS), 0)
    return row, onehot(row == mode_code), quant_code


def expand_pairs(first, last, count, tiles, columns, codes, stage, op, ready):
    row, mode_hot, quant_code = codes
    flux = split2(jnp.concatenate([columns[0:128, :].T[0:16, :], columns[128:256, :].T[0:16, :]], axis=1))
    for k in range(0, count, 2):
        width = ROWS * min(2, count - k)
        at = first + k
        pair = split2(jnp.concatenate([tiles[at], tiles[min(at + 1, last)]], axis=1))
        quant_hot = onehot(row == quant_code + 16 * at)
        spread = dot(pair[0], mode_hot) + dot(pair[1], mode_hot)
        scale = dot(flux[0], quant_hot) + dot(flux[1], quant_hot)
        for p in range(QUANT):
            stage[MODES * p : MODES * (p + 1), 0:width] = spread[0:MODES, 0:width] * scale[p : p + 1, 0:width]
        high, low = split2(stage[:, 0:width])
        op[0:ROWS, ROWS * k : ROWS * k + width] = high
        op[ROWS:, ROWS * k : ROWS * k + width] = low
        ready(slice(ROWS * k, ROWS * k + -(-width // 128) * 128))


def taylor_operator_kernel(stiffness, star, op, tiles, square, columns, stage):
    tiles[...] = jnp.zeros(tiles.shape, F32)
    square[...] = jnp.zeros(square.shape, F32)
    columns[...] = jnp.zeros(columns.shape, F32)
    stage[FEAT:ROWS, :] = jnp.zeros((ROWS - FEAT, stage.shape[1]), F32)
    for c in range(3):
        square[0:MODES, 0:MODES] = -stiffness[c]
        tiles[c] = square[...].T[0:48, :]
        columns[16 * c : 16 * c + QUANT, 0:QUANT] = star[:, c, :]
    expand_pairs(0, 2, 3, tiles, columns, pair_codes(), stage, op, lambda lanes: None)


def operator_kernel(
    stiffness, minus, plus, star, solver_minus, solver_plus, c_out, b_out,
    k_in, m_in, p_in, s_in, sm_in, sp_in, tiles, columns, stage, c_op, b_op, loads, done,
):
    copies = fetch(
        [
            (stiffness, k_in), (minus, m_in), (plus, p_in), (star, s_in),
            (solver_minus, sm_in), (solver_plus, sp_in),
        ],
        loads,
    )
    codes = pair_codes()
    tiles[...] = jnp.zeros(tiles.shape, F32)
    columns[...] = jnp.zeros(columns.shape, F32)
    stage[FEAT:ROWS, :] = jnp.zeros((ROWS - FEAT, stage.shape[1]), F32)
    for copy in copies:
        copy.wait()
    for c in range(3):
        tiles[c, 0:MODES, 0:MODES] = k_in[c]
        columns[16 * c : 16 * c + QUANT, 0:QUANT] = s_in[:, c, :]
    for f in range(4):
        tiles[3 + f, 0:MODES, 0:MODES] = -m_in[:, f, :]
        tiles[7 + f, 0:MODES, 0:MODES] = -p_in[:, f, :]
        columns[16 * (3 + f) : 16 * (3 + f) + QUANT, 0:QUANT] = sm_in[:, f, :]
        columns[16 * (7 + f) : 16 * (7 + f) + QUANT, 0:QUANT] = sp_in[:, f, :]
    sent = []

    def leave(op, out):
        return lambda lanes: sent.extend(fetch([(op.at[:, lanes], out.at[:, lanes])], done, len(sent)))

    expand_pairs(0, 10, 7, tiles, columns, codes, stage, c_op, leave(c_op, c_out))
    expand_pairs(7, 10, 4, tiles, columns, codes, stage, b_op, leave(b_op, b_out))
    for copy in sent:
        copy.wait()


def order_faces(faces):
    digits = jnp.concatenate([faces >> 4, faces & 15], axis=0).astype(F32).astype(BF16)
    from_slot = iota((SLOTS, SLOTS), 0)
    to_slot = iota((SLOTS, SLOTS), 1)
    moved = dot(digits, onehot(from_slot == (to_slot & 127) * CAP + (to_slot >> 7))).astype(jnp.int32)
    return moved[0:4, :] * 16 + moved[4:8, :]


def taylor(start, extras, d_op, pieces, factor_sets):
    cuts = [(0, 256), (256, SLOTS)]
    current = [start[:, lo:hi] for lo, hi in cuts]
    sums = [[value * factors[0] for value in current] for factors in factor_sets]
    for k in range(1, ORDER):
        for i, (lo, hi) in enumerate(cuts):
            for c in range(3):
                put(pieces[i], c, current[i] * extras[c : c + 1, lo:hi])
            current[i] = product(d_op, pieces[i])
            for total, factors in zip(sums, factor_sets):
                total[i] = total[i] + current[i] * factors[k]
    return [jnp.concatenate(total, axis=1) for total in sums]


def order_picks(listed, picks):
    value = listed
    digits = jnp.concatenate([value >> 4, value & 15], axis=0).astype(F32).astype(BF16)
    spread = dot(digits, onehot(iota((128, 128), 0) == (iota((128, 128), 1) >> 3))).astype(jnp.int32)
    spread = spread[0:8, :] * 16 + spread[8:16, :]
    lane = iota((1, 128), 1)
    part = jnp.where(lane < 64, lane & 7, 8)

    def choose(*moves):
        line = jnp.full((1, 128), -1, jnp.int32)
        for ghost, spot in moves:
            line = jnp.where(part == spot, spread[ghost : ghost + 1, :], line)
        return line

    picks[...] = jnp.full(picks.shape, -1, jnp.int32)
    picks[0:1, :] = choose(*[(i, i) for i in range(GHOSTS)])
    picks[1:2, :] = choose((0, 6), (2, 7))
    picks[2:3, :] = choose((1, 6), (3, 7))
    picks[3:4, :] = choose((4, 6))
    picks[4:5, :] = choose((5, 6))


def send_ghosts(value, picks, odd, even):
    slot = iota((SLOTS, 128), 0)
    slot = (slot & 127) * CAP + (slot >> 7)
    base = onehot(slot == picks[0:1, :])
    rest = jnp.concatenate([onehot(slot == picks[k : k + 1, :]) for k in range(1, 5)], axis=1)
    main = dot3(value[0:256, :], base)
    tail = dot3(value[256:320, :], rest)
    first = (main[0:128, :] + jnp.concatenate([tail[:, 0:128], tail[:, 128:256]], axis=0)).T
    second = (main[128:256, :] + jnp.concatenate([tail[:, 256:384], tail[:, 384:512]], axis=0)).T
    for b, step in enumerate(STEPS):
        out = odd if step % 2 else even
        place = 16 * (SENT.index(step) % 4)
        out[place : place + 8, :] = first[8 * b : 8 * b + 8, :]
        out[place + 8 : place + 16, :] = second[8 * b : 8 * b + 8, :]


def relay_kernel(even, twin, up, down, far_up, far_down):
    def piece(rows, step):
        place = 16 * (SENT.index(step) % 4)
        return rows[place : place + 16, :]

    for out, sign in ((up, 1), (down, -1)):
        out[0:16, :] = piece(even, 2 * sign)
        out[16:32, :] = piece(twin, sign)
        out[32:48, :] = piece(twin, 3 * sign)
    for out, sign in ((far_up, 1), (far_down, -1)):
        out[0:16, :] = piece(even, 4 * sign)
        out[16:32, :] = piece(twin, 3 * sign)


def read_ghosts(twin, up, down, far_up, far_down, core):
    even = core == 0
    places = {
        2: (up, 0, up, 0), -2: (down, 0, down, 0), 4: (far_up, 0, far_up, 0), -4: (far_down, 0, far_down, 0),
        1: (up, 16, twin, 0), -1: (twin, 16, down, 16), 3: (far_up, 16, up, 32), -3: (down, 32, far_down, 16),
    }
    firsts, seconds = [], []
    for step in STEPS:
        a, i, b, j = places[step]
        firsts.append(jnp.where(even, a[i : i + 8, :], b[j : j + 8, :]))
        seconds.append(jnp.where(even, a[i + 8 : i + 16, :], b[j + 8 : j + 16, :]))
    blank = jnp.zeros((64, 128), F32)
    first = jnp.concatenate(firsts + [blank], axis=0).T
    second = jnp.concatenate(seconds + [blank], axis=0).T
    row = iota((128, 128), 0)
    col = iota((128, 128), 1)
    part = col & 7
    group = col - part
    halves = [first[0:64, :], first[64:128, :], second[0:64, :], second[64:128, :]]
    places = [((0, 6), (2, 7)), ((1, 6), (3, 7)), ((4, 6),), ((5, 6),)]
    tail = None
    for half, moves in zip(halves, places):
        hit = None
        for ghost, spot in moves:
            one = (part == ghost) & (row == group + spot)
            hit = one if hit is None else hit | one
        term = dot3(half, onehot(hit))
        tail = term if tail is None else tail + term
    return jnp.concatenate([first, second, tail], axis=0)


def remote_flux(value, ghosts, extras, faces, b_op, both):
    high, low = split2(jnp.concatenate([value, ghosts], axis=1))
    row = iota((512, 128), 0)
    beyond = row - SLOTS
    local = (row & 127) * CAP + (row >> 7)
    spot = beyond & 7
    ghost = jnp.where((spot < GHOSTS) & (beyond < 64), SLOTS + (beyond >> 3) * GHOSTS + spot, -1)
    code = jnp.where(row < SLOTS, local, ghost)
    for f in range(4):
        hot = jnp.concatenate(
            [onehot(code == faces[f : f + 1, 128 * k : 128 * (k + 1)]) for k in range(3)], axis=1
        )
        picked = (dot(high, hot) + dot(low, hot)) * extras[3 + f : 4 + f, :]
        put(both, f, picked)
    return product(b_op, both)


def fetch(pairs, done, base=0):
    copies = [pltpu.make_async_copy(src, dst, done.at[base + k]) for k, (src, dst) in enumerate(pairs)]
    for copy in copies:
        copy.start()
    return copies


def occupied(extras):
    return jnp.where(extras[7:8, :] > 0.5, 1.0, 0.0)


def unpack_kernel(recv, tables, state, extras, picks, stage):
    order_picks(tables[8:16, 0:128], picks)
    unpack_rows(recv, stage)
    for t in range(CAP):
        extras[:, 128 * t : 128 * (t + 1)] = stage[STRIDE * t : STRIDE * t + 8, :]
        state[:, 128 * t : 128 * (t + 1)] = stage[STRIDE * t + 8 : STRIDE * t + 8 + ROWS, :]


def start_kernel(state, extras, picks, d_op, first, later, odd, even, one_piece, other_piece):
    one, two = taylor(
        state[...], extras, d_op, (one_piece, other_piece), [weights_of(0.0, 1.0), weights_of(1.0, 2.0)]
    )
    first[...] = one
    later[...] = two
    send_ghosts(first, picks, odd, even)


def local_kernel(state, value, extras, c_op, faces, out, order, both):
    order[...] = order_faces(faces[0:4, :])
    local_terms(state, value, extras, c_op, out, both)


def local_terms(state, value, extras, c_op, out, both):
    for k in range(7):
        put(both, k, value[...] * extras[k : k + 1, :])
    change = product(c_op, both)
    out[...] = state[...] + occupied(extras) * change


def middle_kernel(
    core, twin, up, down, far_up, far_down, partial, first, later, extras, faces, picks, d_op, b_op,
    middle, second, odd, even, one_piece, other_piece, wide,
):
    table = read_ghosts(twin, up, down, far_up, far_down, core[0])
    flux = remote_flux(first[...], table, extras, faces, b_op, wide)
    middle[...] = partial[...] + occupied(extras) * flux
    (fresh,) = taylor(middle[...], extras, d_op, (one_piece, other_piece), [weights_of(0.0, 1.0)])
    second[...] = jnp.where(extras[7:8, :] > 1.5, later[...], fresh)
    send_ghosts(second, picks, odd, even)


def final_kernel(
    core, twin, up, down, far_up, far_down, partial, second, extras, faces, b_op, out, stage, wide
):
    table = read_ghosts(twin, up, down, far_up, far_down, core[0])
    flux = remote_flux(second[...], table, extras, faces, b_op, wide)
    final = partial[...] + occupied(extras) * flux
    stage[...] = jnp.zeros((CHUNK, DEVS), F32)
    for t in range(CAP):
        stage[STRIDE * t + 8 : STRIDE * t + 8 + ROWS, :] = final[:, 128 * t : 128 * (t + 1)]
    pack_rows(stage, out)


def shape(*dims, dtype=F32):
    return jax.ShapeDtypeStruct(dims, dtype)


def call(kernel, name, outs, scratch, flops, operands, spaces="", out_spaces="", limit=16 * 1024 * 1024):
    kinds = {"s": pltpu.SMEM, "v": pltpu.VMEM, "h": pltpu.HBM}
    spaces = spaces.ljust(len(operands), "v")
    flat = jax.tree.leaves(outs)
    out_specs = [pl.BlockSpec(memory_space=kinds[k]) for k in out_spaces.ljust(len(flat), "v")]
    moved = sum(math.prod(o.shape) * 4 for o in operands)
    return pl.pallas_call(
        kernel,
        name=name,
        out_shape=outs,
        in_specs=[pl.BlockSpec(memory_space=kinds[k]) for k in spaces],
        out_specs=out_specs if isinstance(outs, list) else out_specs[0],
        scratch_shapes=scratch,
        cost_estimate=pl.CostEstimate(flops=flops, bytes_accessed=moved, transcendentals=0),
        compiler_params=pltpu.CompilerParams(vmem_limit_bytes=limit),
    )(*operands)


def vmem(*dims, dtype=F32):
    return pltpu.VMEM(dims, dtype)


def exchange(rows, per):
    cube = rows.reshape(DEVS, per, 128)
    return lax.all_to_all(cube, "dom", split_axis=0, concat_axis=0, tiled=True).reshape(DEVS * per, 128)


def swap_ghosts(odd, even, value):
    def move(part, shift):
        pairs = [(device_of(o), device_of((o + shift) % DEVS)) for o in range(DEVS)]
        return lax.ppermute(part, "dom", pairs)

    twins = [(device_of(o), device_of(o ^ 1)) for o in range(DEVS)]
    twin = lax.ppermute(odd, "dom", twins)
    parts = call(
        relay_kernel, "relay", [shape(48, 128), shape(48, 128), shape(32, 128), shape(32, 128)], [], 10**6, (even, twin)
    )
    value, parts = lax.optimization_barrier((value, parts))
    return (twin, *[move(part, shift) for part, shift in zip(parts, (2, -2, 4, -4))]), value


def local(
    modal_dofs, jacobian, face_area, cluster_id, target_slot, ghost_slots, face_neighbours,
    stiffness, star_matrix, face_minus, face_plus, solver_minus, solver_plus,
):
    core = (lax.axis_index("dom").astype(jnp.int32) & 1).reshape(1)
    target = target_slot.reshape(1, BLOCK)
    sent, tables = call(
        scatter_kernel, "scatter", [shape(CHUNK, DEVS), shape(16, SLOTS, dtype=jnp.int32)],
        [
            vmem(QUANT, MODES, BLOCK), vmem(328, BLOCK), vmem(CHUNK, DEVS), vmem(1, BLOCK, dtype=jnp.int32),
            vmem(1, BLOCK, dtype=jnp.int32), vmem(6, 1, NEIGH, dtype=jnp.int32), pltpu.SemaphoreType.DMA((7,)),
        ],
        10**8,
        (
            core, jnp.transpose(modal_dofs, (1, 0, 2)), jacobian, face_area, cluster_id.reshape(1, BLOCK), target,
            face_neighbours, jnp.transpose(ghost_slots, (2, 0, 1)),
        ),
        "shhhhhhh", "", FULL,
    )
    received = exchange(sent, 8)

    star, minus, plus, solve_minus, solve_plus = [
        jnp.transpose(a, (1, 0, 2)) for a in (star_matrix, face_minus, face_plus, solver_minus, solver_plus)
    ]
    c_op, b_op = call(
        operator_kernel, "operators",
        [shape(2 * ROWS, w, dtype=BF16) for w in (2304, 1280)],
        [
            vmem(3, MODES, MODES), vmem(MODES, 4, MODES), vmem(MODES, 4, MODES),
            vmem(QUANT, 3, QUANT), vmem(QUANT, 4, QUANT), vmem(QUANT, 4, QUANT),
            vmem(11, 48, 128), vmem(256, 128), vmem(ROWS, 2 * ROWS), vmem(2 * ROWS, 2304, dtype=BF16),
            vmem(2 * ROWS, 1280, dtype=BF16), pltpu.SemaphoreType.DMA((6,)), pltpu.SemaphoreType.DMA((6,)),
        ],
        10**9, (stiffness, minus, plus, star, solve_minus, solve_plus), "hhhhhh", "hh", FULL - 1900 * 1024,
    )
    stiffness, star, _ = lax.optimization_barrier((stiffness, star, b_op))
    d_op = call(
        taylor_operator_kernel, "taylor_operators", shape(2 * ROWS, 960, dtype=BF16),
        [vmem(3, 48, 128), vmem(128, 128), vmem(256, 128), vmem(ROWS, 2 * ROWS)],
        10**9, (stiffness, star),
    )
    home = [(o, device_of(o)) for o in range(DEVS)]
    tables = lax.ppermute(tables, "dom", home)
    received, tables = lax.optimization_barrier((received, tables))
    x_scratch = [vmem(3 * ROWS, 512, dtype=BF16), vmem(3 * ROWS, 256, dtype=BF16)]
    y_scratch = [vmem(4 * ROWS, 2 * SLOTS, dtype=BF16)]
    z_scratch = [vmem(7 * ROWS, 2 * SLOTS, dtype=BF16)]
    field = shape(ROWS, SLOTS)
    halo = [shape(64, 128)] * 2
    state, extras, picks = call(
        unpack_kernel, "unpack", [field, shape(8, SLOTS), shape(8, 128, dtype=jnp.int32)],
        [vmem(CHUNK, DEVS)], 10**8, (received, tables),
    )
    first, later, odd, even = call(
        start_kernel, "start", [field, field, *halo], x_scratch, 10**9, (state, extras, picks, d_op),
    )
    ghosts, first = swap_ghosts(odd, even, first)
    partial1, faces = call(
        local_kernel, "local1", [field, shape(4, SLOTS, dtype=jnp.int32)], z_scratch, 10**9,
        (state, first, extras, c_op, tables),
    )
    middle, second, odd, even = call(
        middle_kernel, "middle", [field, field, *halo],
        x_scratch + y_scratch, 2 * 10**9,
        (core, *ghosts, partial1, first, later, extras, faces, picks, d_op, b_op), "s",
    )
    ghosts, second = swap_ghosts(odd, even, second)
    partial2 = call(
        local_terms, "local2", field, z_scratch, 10**9, (middle, second, extras, c_op)
    )
    back = call(
        final_kernel, "final", shape(CHUNK, DEVS),
        [vmem(CHUNK, DEVS)] + y_scratch, 10**9,
        (core, *ghosts, partial2, second, extras, faces, b_op), "s",
    )
    returned = exchange(back, 8)
    result = call(
        gather_kernel, "gather", shape(QUANT, MODES, BLOCK), [vmem(CHUNK, DEVS)], 10**8, (returned, target)
    )
    return jnp.transpose(result, (1, 0, 2))


def solution(mesh):
    placed = (
        P(None, None, "dom"), P(None, "dom"), P(None, "dom"), P("dom"), P("dom"), P("dom", None, None),
        P(None, "dom"), P(), P(), P(), P(), P(), P(),
    )
    return jax.shard_map(
        local, mesh=mesh, in_specs=placed, out_specs=P(None, None, "dom"), check_vma=False
    )
```

```python
import math

import jax
import jax.numpy as jnp
from jax import lax
from jax.experimental import pallas as pl
from jax.experimental.pallas import tpu as pltpu
from jax.sharding import PartitionSpec as P

ORDER = 5
MODES = 35
QUANT = 9
FEAT = MODES * QUANT
ROWS = 320
BLOCK = 256
DEVS = 128
CAP = 3
SLOTS = 384
STRIDE = 336
CHUNK = 1024
GHOSTS = 6
NEIGH = 8
STEPS = (1, -1, 2, -2, 3, -3, 4, -4)
SENT = (1, -1, 3, -3, 2, -2, 4, -4)
F32 = jnp.float32
BF16 = jnp.bfloat16
FULL = 67043328


def weights_of(lower, upper):
    return [(upper ** (k + 1) - lower ** (k + 1)) / math.factorial(k + 1) for k in range(ORDER)]


def dot(a, b):
    return jnp.dot(a, b, preferred_element_type=F32)


def split2(x):
    high = x.astype(BF16)
    return high, (x - high.astype(F32)).astype(BF16)


def split3(x):
    high = x.astype(BF16)
    rest = x - high.astype(F32)
    mid = rest.astype(BF16)
    return high, mid, (rest - mid.astype(F32)).astype(BF16)


def dot3(a, b, dims=None):
    total = None
    for part in split3(a):
        if dims is None:
            term = dot(part, b)
        else:
            term = lax.dot_general(part, b, (dims, ((), ())), preferred_element_type=F32)
        total = term if total is None else total + term
    return total


def dot2(a, b):
    high, low = split2(a)
    return dot(high, b) + dot(low, b)


def product(op, both):
    depth, width = both.shape[0], both.shape[1] // 2
    wide = dot(op[0:ROWS, 0:depth], both[...])
    return wide[:, 0:width] + wide[:, width:] + dot(op[ROWS:, 0:depth], both[:, 0:width])


def put(both, at, value):
    width = both.shape[1] // 2
    high, low = split2(value)
    both[ROWS * at : ROWS * (at + 1), 0:width] = high
    both[ROWS * at : ROWS * (at + 1), width:] = low


PATH = (0, 1, 2, 3, 7, 11, 15, 14, 10, 6, 5, 9, 13, 12, 8, 4)


def owner_of(device):
    group = device >> 3
    place = jnp.zeros_like(group)
    for k, g in enumerate(PATH):
        place = jnp.where(group == g, k, place)
    inner = device & 7
    return place * 8 + jnp.where((place & 1) > 0, inner ^ 6, inner)


def device_of(owner):
    group = owner // 8
    return PATH[group] * 8 + (owner % 8 ^ (6 if group % 2 else 0))


def iota(shape, dim):
    return lax.broadcasted_iota(jnp.int32, shape, dim)


def onehot(condition):
    return jnp.where(condition, 1.0, 0.0).astype(BF16)


def pack_rows(stage, out_ref):
    for k in range(8):
        out_ref[pl.ds(k, DEVS, stride=8), :] = stage[128 * k : 128 * k + 128, :].T


def unpack_rows(recv_ref, stage):
    for k in range(8):
        stage[128 * k : 128 * k + 128, :] = recv_ref[pl.ds(k, DEVS, stride=8), :].T


def scatter_kernel(
    core, modal, jac, area, cluster, target, faces, listed, out, tables, cells, values, stage, kinds, places, lists, done
):
    copies = [
        pltpu.make_async_copy(modal, cells, done.at[0]),
        pltpu.make_async_copy(jac, values.at[0:3, :], done.at[1]),
        pltpu.make_async_copy(area, values.at[3:7, :], done.at[2]),
        pltpu.make_async_copy(cluster, kinds, done.at[3]),
        pltpu.make_async_copy(target, places, done.at[4]),
        pltpu.make_async_copy(faces, tables.at[0:4, :], done.at[5]),
        pltpu.make_async_copy(listed, lists, done.at[6]),
    ]
    for copy in copies:
        copy.start()
    copies[4].wait()
    half = owner_of(iota((DEVS, DEVS), 0)) * CAP
    slot = jnp.concatenate([half, half], axis=1)
    wanted = places[...]
    hots = [onehot(slot + t == wanted) for t in range(CAP)]
    tables[8:16, :] = jnp.zeros((8, SLOTS), jnp.int32)
    values[320:328, :] = jnp.zeros((8, BLOCK), F32)
    stage[CAP * STRIDE :, :] = jnp.zeros((CHUNK - CAP * STRIDE, DEVS), F32)
    for t in range(CAP):
        stage[STRIDE * t + 328 : STRIDE * (t + 1), :] = jnp.zeros((8, DEVS), F32)
    for k in (0, 1, 2, 3, 5, 6):
        copies[k].wait()
    tables[4:8, :] = jnp.full((4, SLOTS), core[0], jnp.int32)
    for i in range(GHOSTS):
        tables[8 + i : 9 + i, 0:NEIGH] = lists[i]
    values[7:8, :] = 1.0 + kinds[...].astype(F32)
    for q in range(QUANT):
        values[8 + MODES * q : 8 + MODES * (q + 1), :] = cells[q]
    parts = split3(values[...])
    for t in range(CAP):
        total = None
        for part in parts:
            term = lax.dot_general(part, hots[t], (((1,), (1,)), ((), ())), preferred_element_type=F32)
            total = term if total is None else total + term
        stage[STRIDE * t : STRIDE * t + 328, :] = total
    pack_rows(stage, out)


def gather_kernel(recv, target, out, stage):
    unpack_rows(recv, stage)
    wanted = target[...]
    half = owner_of(iota((DEVS, DEVS), 0)) * CAP
    slot = jnp.concatenate([half, half], axis=1)
    total = None
    for t in range(CAP):
        part = stage[STRIDE * t + 8 : STRIDE * t + 8 + ROWS, :]
        term = dot3(part, onehot(slot + t == wanted))
        total = term if total is None else total + term
    for q in range(QUANT):
        out[q] = total[MODES * q : MODES * (q + 1), :]


def pair_codes():
    col = iota((8, 2 * ROWS), 1)
    second = jnp.where(col >= ROWS, 1, 0)
    inner = col - second * ROWS
    quant = (inner * 1873) >> 16
    mode = inner - quant * MODES
    valid = inner < FEAT
    mode_code = jnp.where(valid, second * 128 + mode, -1)[0:1]
    quant_code = jnp.where(valid, second * 16 + quant, -512)[0:1]
    row = iota((256, 2 * ROWS), 0)
    return row, onehot(row == mode_code), quant_code


def expand_pairs(first, last, count, tiles, columns, codes, stage, op, ready):
    row, mode_hot, quant_code = codes
    flux = split2(jnp.concatenate([columns[0:128, :].T[0:16, :], columns[128:256, :].T[0:16, :]], axis=1))
    for k in range(0, count, 2):
        width = ROWS * min(2, count - k)
        at = first + k
        pair = split2(jnp.concatenate([tiles[at], tiles[min(at + 1, last)]], axis=1))
        quant_hot = onehot(row == quant_code + 16 * at)
        spread = dot(pair[0], mode_hot) + dot(pair[1], mode_hot)
        scale = dot(flux[0], quant_hot) + dot(flux[1], quant_hot)
        for p in range(QUANT):
            stage[MODES * p : MODES * (p + 1), 0:width] = spread[0:MODES, 0:width] * scale[p : p + 1, 0:width]
        high, low = split2(stage[:, 0:width])
        op[0:ROWS, ROWS * k : ROWS * k + width] = high
        op[ROWS:, ROWS * k : ROWS * k + width] = low
        ready(slice(ROWS * k, ROWS * k + -(-width // 128) * 128))


def taylor_operator_kernel(stiffness, star, op, tiles, square, columns, stage):
    tiles[...] = jnp.zeros(tiles.shape, F32)
    square[...] = jnp.zeros(square.shape, F32)
    columns[...] = jnp.zeros(columns.shape, F32)
    stage[FEAT:ROWS, :] = jnp.zeros((ROWS - FEAT, stage.shape[1]), F32)
    for c in range(3):
        square[0:MODES, 0:MODES] = -stiffness[c]
        tiles[c] = square[...].T[0:48, :]
        columns[16 * c : 16 * c + QUANT, 0:QUANT] = star[:, c, :]
    expand_pairs(0, 2, 3, tiles, columns, pair_codes(), stage, op, lambda lanes: None)


def operator_kernel(
    stiffness, minus, plus, star, solver_minus, solver_plus, c_out, b_out,
    k_in, m_in, p_in, s_in, sm_in, sp_in, tiles, columns, stage, c_op, b_op, loads, done,
):
    copies = fetch(
        [
            (stiffness, k_in), (minus, m_in), (plus, p_in), (star, s_in),
            (solver_minus, sm_in), (solver_plus, sp_in),
        ],
        loads,
    )
    codes = pair_codes()
    tiles[...] = jnp.zeros(tiles.shape, F32)
    columns[...] = jnp.zeros(columns.shape, F32)
    stage[FEAT:ROWS, :] = jnp.zeros((ROWS - FEAT, stage.shape[1]), F32)
    for copy in copies:
        copy.wait()
    for c in range(3):
        tiles[c, 0:MODES, 0:MODES] = k_in[c]
        columns[16 * c : 16 * c + QUANT, 0:QUANT] = s_in[:, c, :]
    for f in range(4):
        tiles[3 + f, 0:MODES, 0:MODES] = -m_in[:, f, :]
        tiles[7 + f, 0:MODES, 0:MODES] = -p_in[:, f, :]
        columns[16 * (3 + f) : 16 * (3 + f) + QUANT, 0:QUANT] = sm_in[:, f, :]
        columns[16 * (7 + f) : 16 * (7 + f) + QUANT, 0:QUANT] = sp_in[:, f, :]
    sent = []

    def leave(op, out):
        return lambda lanes: sent.extend(fetch([(op.at[:, lanes], out.at[:, lanes])], done, len(sent)))

    expand_pairs(0, 10, 7, tiles, columns, codes, stage, c_op, leave(c_op, c_out))
    expand_pairs(7, 10, 4, tiles, columns, codes, stage, b_op, leave(b_op, b_out))
    for copy in sent:
        copy.wait()


def order_faces(faces):
    digits = jnp.concatenate([faces >> 4, faces & 15], axis=0).astype(F32).astype(BF16)
    from_slot = iota((SLOTS, SLOTS), 0)
    to_slot = iota((SLOTS, SLOTS), 1)
    moved = dot(digits, onehot(from_slot == (to_slot & 127) * CAP + (to_slot >> 7))).astype(jnp.int32)
    return moved[0:4, :] * 16 + moved[4:8, :]


def taylor(start, extras, d_op, pieces, factor_sets):
    cuts = [(0, 256), (256, SLOTS)]
    current = [start[:, lo:hi] for lo, hi in cuts]
    sums = [[value * factors[0] for value in current] for factors in factor_sets]
    for k in range(1, ORDER):
        for i, (lo, hi) in enumerate(cuts):
            for c in range(3):
                put(pieces[i], c, current[i] * extras[c : c + 1, lo:hi])
            current[i] = product(d_op, pieces[i])
            for total, factors in zip(sums, factor_sets):
                total[i] = total[i] + current[i] * factors[k]
    return [jnp.concatenate(total, axis=1) for total in sums]


def order_picks(listed, picks):
    value = listed
    digits = jnp.concatenate([value >> 4, value & 15], axis=0).astype(F32).astype(BF16)
    spread = dot(digits, onehot(iota((128, 128), 0) == (iota((128, 128), 1) >> 3))).astype(jnp.int32)
    spread = spread[0:8, :] * 16 + spread[8:16, :]
    lane = iota((1, 128), 1)
    part = jnp.where(lane < 64, lane & 7, 8)

    def choose(*moves):
        line = jnp.full((1, 128), -1, jnp.int32)
        for ghost, spot in moves:
            line = jnp.where(part == spot, spread[ghost : ghost + 1, :], line)
        return line

    picks[...] = jnp.full(picks.shape, -1, jnp.int32)
    picks[0:1, :] = choose(*[(i, i) for i in range(GHOSTS)])
    picks[1:2, :] = choose((0, 6), (2, 7))
    picks[2:3, :] = choose((1, 6), (3, 7))
    picks[3:4, :] = choose((4, 6))
    picks[4:5, :] = choose((5, 6))


def send_ghosts(value, picks, odd, even):
    slot = iota((SLOTS, 128), 0)
    slot = (slot & 127) * CAP + (slot >> 7)
    base = onehot(slot == picks[0:1, :])
    rest = jnp.concatenate([onehot(slot == picks[k : k + 1, :]) for k in range(1, 5)], axis=1)
    main = dot2(value[0:256, :], base)
    tail = dot2(value[256:320, :], rest)
    first = (main[0:128, :] + jnp.concatenate([tail[:, 0:128], tail[:, 128:256]], axis=0)).T
    second = (main[128:256, :] + jnp.concatenate([tail[:, 256:384], tail[:, 384:512]], axis=0)).T
    for b, step in enumerate(STEPS):
        out = odd if step % 2 else even
        place = 16 * (SENT.index(step) % 4)
        out[place : place + 8, :] = first[8 * b : 8 * b + 8, :]
        out[place + 8 : place + 16, :] = second[8 * b : 8 * b + 8, :]


def relay_kernel(even, twin, up, down, far_up, far_down):
    def piece(rows, step):
        place = 16 * (SENT.index(step) % 4)
        return rows[place : place + 16, :]

    for out, sign in ((up, 1), (down, -1)):
        out[0:16, :] = piece(even, 2 * sign)
        out[16:32, :] = piece(twin, sign)
        out[32:48, :] = piece(twin, 3 * sign)
    for out, sign in ((far_up, 1), (far_down, -1)):
        out[0:16, :] = piece(even, 4 * sign)
        out[16:32, :] = piece(twin, 3 * sign)


def read_ghosts(twin, up, down, far_up, far_down, core):
    even = core == 0
    places = {
        2: (up, 0, up, 0), -2: (down, 0, down, 0), 4: (far_up, 0, far_up, 0), -4: (far_down, 0, far_down, 0),
        1: (up, 16, twin, 0), -1: (twin, 16, down, 16), 3: (far_up, 16, up, 32), -3: (down, 32, far_down, 16),
    }
    firsts, seconds = [], []
    for step in STEPS:
        a, i, b, j = places[step]
        firsts.append(jnp.where(even, a[i : i + 8, :], b[j : j + 8, :]))
        seconds.append(jnp.where(even, a[i + 8 : i + 16, :], b[j + 8 : j + 16, :]))
    blank = jnp.zeros((64, 128), F32)
    first = jnp.concatenate(firsts + [blank], axis=0).T
    second = jnp.concatenate(seconds + [blank], axis=0).T
    row = iota((128, 128), 0)
    col = iota((128, 128), 1)
    part = col & 7
    group = col - part
    halves = [first[0:64, :], first[64:128, :], second[0:64, :], second[64:128, :]]
    places = [((0, 6), (2, 7)), ((1, 6), (3, 7)), ((4, 6),), ((5, 6),)]
    tail = None
    for half, moves in zip(halves, places):
        hit = None
        for ghost, spot in moves:
            one = (part == ghost) & (row == group + spot)
            hit = one if hit is None else hit | one
        term = dot2(half, onehot(hit))
        tail = term if tail is None else tail + term
    return jnp.concatenate([first, second, tail], axis=0)


def remote_flux(value, ghosts, extras, faces, b_op, both):
    high, low = split2(jnp.concatenate([value, ghosts], axis=1))
    row = iota((512, 128), 0)
    beyond = row - SLOTS
    local = (row & 127) * CAP + (row >> 7)
    spot = beyond & 7
    ghost = jnp.where((spot < GHOSTS) & (beyond < 64), SLOTS + (beyond >> 3) * GHOSTS + spot, -1)
    code = jnp.where(row < SLOTS, local, ghost)
    for f in range(4):
        hot = jnp.concatenate(
            [onehot(code == faces[f : f + 1, 128 * k : 128 * (k + 1)]) for k in range(3)], axis=1
        )
        picked = (dot(high, hot) + dot(low, hot)) * extras[3 + f : 4 + f, :]
        put(both, f, picked)
    return product(b_op, both)


def fetch(pairs, done, base=0):
    copies = [pltpu.make_async_copy(src, dst, done.at[base + k]) for k, (src, dst) in enumerate(pairs)]
    for copy in copies:
        copy.start()
    return copies


def occupied(extras):
    return jnp.where(extras[7:8, :] > 0.5, 1.0, 0.0)


def unpack_kernel(recv, tables, state, extras, picks, stage):
    order_picks(tables[8:16, 0:128], picks)
    unpack_rows(recv, stage)
    for t in range(CAP):
        extras[:, 128 * t : 128 * (t + 1)] = stage[STRIDE * t : STRIDE * t + 8, :]
        state[:, 128 * t : 128 * (t + 1)] = stage[STRIDE * t + 8 : STRIDE * t + 8 + ROWS, :]


def start_kernel(state, extras, picks, d_op, first, later, odd, even, one_piece, other_piece):
    one, two = taylor(
        state[...], extras, d_op, (one_piece, other_piece), [weights_of(0.0, 1.0), weights_of(1.0, 2.0)]
    )
    first[...] = one
    later[...] = two
    send_ghosts(first, picks, odd, even)


def local_kernel(state, value, extras, c_op, faces, out, order, both):
    order[...] = order_faces(faces[0:4, :])
    local_terms(state, value, extras, c_op, out, both)


def local_terms(state, value, extras, c_op, out, both):
    for k in range(7):
        put(both, k, value[...] * extras[k : k + 1, :])
    change = product(c_op, both)
    out[...] = state[...] + occupied(extras) * change


def middle_kernel(
    core, twin, up, down, far_up, far_down, partial, first, later, extras, faces, picks, d_op, b_op,
    middle, second, odd, even, one_piece, other_piece, wide,
):
    table = read_ghosts(twin, up, down, far_up, far_down, core[0])
    flux = remote_flux(first[...], table, extras, faces, b_op, wide)
    middle[...] = partial[...] + occupied(extras) * flux
    (fresh,) = taylor(middle[...], extras, d_op, (one_piece, other_piece), [weights_of(0.0, 1.0)])
    second[...] = jnp.where(extras[7:8, :] > 1.5, later[...], fresh)
    send_ghosts(second, picks, odd, even)


def final_kernel(
    core, twin, up, down, far_up, far_down, partial, second, extras, faces, b_op, out, stage, wide
):
    table = read_ghosts(twin, up, down, far_up, far_down, core[0])
    flux = remote_flux(second[...], table, extras, faces, b_op, wide)
    final = partial[...] + occupied(extras) * flux
    stage[...] = jnp.zeros((CHUNK, DEVS), F32)
    for t in range(CAP):
        stage[STRIDE * t + 8 : STRIDE * t + 8 + ROWS, :] = final[:, 128 * t : 128 * (t + 1)]
    pack_rows(stage, out)


def shape(*dims, dtype=F32):
    return jax.ShapeDtypeStruct(dims, dtype)


def call(kernel, name, outs, scratch, flops, operands, spaces="", out_spaces="", limit=16 * 1024 * 1024):
    kinds = {"s": pltpu.SMEM, "v": pltpu.VMEM, "h": pltpu.HBM}
    spaces = spaces.ljust(len(operands), "v")
    flat = jax.tree.leaves(outs)
    out_specs = [pl.BlockSpec(memory_space=kinds[k]) for k in out_spaces.ljust(len(flat), "v")]
    moved = sum(math.prod(o.shape) * 4 for o in operands)
    return pl.pallas_call(
        kernel,
        name=name,
        out_shape=outs,
        in_specs=[pl.BlockSpec(memory_space=kinds[k]) for k in spaces],
        out_specs=out_specs if isinstance(outs, list) else out_specs[0],
        scratch_shapes=scratch,
        cost_estimate=pl.CostEstimate(flops=flops, bytes_accessed=moved, transcendentals=0),
        compiler_params=pltpu.CompilerParams(vmem_limit_bytes=limit),
    )(*operands)


def vmem(*dims, dtype=F32):
    return pltpu.VMEM(dims, dtype)


def exchange(rows, per):
    cube = rows.reshape(DEVS, per, 128)
    return lax.all_to_all(cube, "dom", split_axis=0, concat_axis=0, tiled=True).reshape(DEVS * per, 128)


def swap_ghosts(odd, even, value):
    def move(part, shift):
        pairs = [(device_of(o), device_of((o + shift) % DEVS)) for o in range(DEVS)]
        return lax.ppermute(part, "dom", pairs)

    twins = [(device_of(o), device_of(o ^ 1)) for o in range(DEVS)]
    twin = lax.ppermute(odd, "dom", twins)
    parts = call(
        relay_kernel, "relay", [shape(48, 128), shape(48, 128), shape(32, 128), shape(32, 128)], [], 10**6, (even, twin)
    )
    value, parts = lax.optimization_barrier((value, parts))
    return (twin, *[move(part, shift) for part, shift in zip(parts, (2, -2, 4, -4))]), value


def local(
    modal_dofs, jacobian, face_area, cluster_id, target_slot, ghost_slots, face_neighbours,
    stiffness, star_matrix, face_minus, face_plus, solver_minus, solver_plus,
):
    core = (lax.axis_index("dom").astype(jnp.int32) & 1).reshape(1)
    target = target_slot.reshape(1, BLOCK)
    sent, tables = call(
        scatter_kernel, "scatter", [shape(CHUNK, DEVS), shape(16, SLOTS, dtype=jnp.int32)],
        [
            vmem(QUANT, MODES, BLOCK), vmem(328, BLOCK), vmem(CHUNK, DEVS), vmem(1, BLOCK, dtype=jnp.int32),
            vmem(1, BLOCK, dtype=jnp.int32), vmem(6, 1, NEIGH, dtype=jnp.int32), pltpu.SemaphoreType.DMA((7,)),
        ],
        10**8,
        (
            core, jnp.transpose(modal_dofs, (1, 0, 2)), jacobian, face_area, cluster_id.reshape(1, BLOCK), target,
            face_neighbours, jnp.transpose(ghost_slots, (2, 0, 1)),
        ),
        "shhhhhhh", "", FULL,
    )
    received = exchange(sent, 8)

    star, minus, plus, solve_minus, solve_plus = [
        jnp.transpose(a, (1, 0, 2)) for a in (star_matrix, face_minus, face_plus, solver_minus, solver_plus)
    ]
    c_op, b_op = call(
        operator_kernel, "operators",
        [shape(2 * ROWS, w, dtype=BF16) for w in (2304, 1280)],
        [
            vmem(3, MODES, MODES), vmem(MODES, 4, MODES), vmem(MODES, 4, MODES),
            vmem(QUANT, 3, QUANT), vmem(QUANT, 4, QUANT), vmem(QUANT, 4, QUANT),
            vmem(11, 48, 128), vmem(256, 128), vmem(ROWS, 2 * ROWS), vmem(2 * ROWS, 2304, dtype=BF16),
            vmem(2 * ROWS, 1280, dtype=BF16), pltpu.SemaphoreType.DMA((6,)), pltpu.SemaphoreType.DMA((6,)),
        ],
        10**9, (stiffness, minus, plus, star, solve_minus, solve_plus), "hhhhhh", "hh", FULL - 1900 * 1024,
    )
    stiffness, star, _ = lax.optimization_barrier((stiffness, star, b_op))
    d_op = call(
        taylor_operator_kernel, "taylor_operators", shape(2 * ROWS, 960, dtype=BF16),
        [vmem(3, 48, 128), vmem(128, 128), vmem(256, 128), vmem(ROWS, 2 * ROWS)],
        10**9, (stiffness, star),
    )
    home = [(o, device_of(o)) for o in range(DEVS)]
    tables = lax.ppermute(tables, "dom", home)
    received, tables = lax.optimization_barrier((received, tables))
    x_scratch = [vmem(3 * ROWS, 512, dtype=BF16), vmem(3 * ROWS, 256, dtype=BF16)]
    y_scratch = [vmem(4 * ROWS, 2 * SLOTS, dtype=BF16)]
    z_scratch = [vmem(7 * ROWS, 2 * SLOTS, dtype=BF16)]
    field = shape(ROWS, SLOTS)
    halo = [shape(64, 128)] * 2
    state, extras, picks = call(
        unpack_kernel, "unpack", [field, shape(8, SLOTS), shape(8, 128, dtype=jnp.int32)],
        [vmem(CHUNK, DEVS)], 10**8, (received, tables),
    )
    first, later, odd, even = call(
        start_kernel, "start", [field, field, *halo], x_scratch, 10**9, (state, extras, picks, d_op),
    )
    ghosts, first = swap_ghosts(odd, even, first)
    partial1, faces = call(
        local_kernel, "local1", [field, shape(4, SLOTS, dtype=jnp.int32)], z_scratch, 10**9,
        (state, first, extras, c_op, tables),
    )
    middle, second, odd, even = call(
        middle_kernel, "middle", [field, field, *halo],
        x_scratch + y_scratch, 2 * 10**9,
        (core, *ghosts, partial1, first, later, extras, faces, picks, d_op, b_op), "s",
    )
    ghosts, second = swap_ghosts(odd, even, second)
    partial2 = call(
        local_terms, "local2", field, z_scratch, 10**9, (middle, second, extras, c_op)
    )
    back = call(
        final_kernel, "final", shape(CHUNK, DEVS),
        [vmem(CHUNK, DEVS)] + y_scratch, 10**9,
        (core, *ghosts, partial2, second, extras, faces, b_op), "s",
    )
    returned = exchange(back, 8)
    result = call(
        gather_kernel, "gather", shape(QUANT, MODES, BLOCK), [vmem(CHUNK, DEVS)], 10**8, (returned, target)
    )
    return jnp.transpose(result, (1, 0, 2))


def solution(mesh):
    placed = (
        P(None, None, "dom"), P(None, "dom"), P(None, "dom"), P("dom"), P("dom"), P("dom", None, None),
        P(None, "dom"), P(), P(), P(), P(), P(), P(),
    )
    return jax.shard_map(
        local, mesh=mesh, in_specs=placed, out_specs=P(None, None, "dom"), check_vma=False
    )
```

```python
import math

import jax
import jax.numpy as jnp
from jax import lax
from jax.experimental import pallas as pl
from jax.experimental.pallas import tpu as pltpu
from jax.sharding import PartitionSpec as P

ORDER = 5
MODES = 35
QUANT = 9
FEAT = MODES * QUANT
ROWS = 320
BLOCK = 256
DEVS = 128
CAP = 3
SLOTS = 384
STRIDE = 336
CHUNK = 1024
GHOSTS = 6
NEIGH = 8
STEPS = (1, -1, 2, -2, 3, -3, 4, -4)
SENT = (1, -1, 3, -3, 2, -2, 4, -4)
F32 = jnp.float32
BF16 = jnp.bfloat16
FULL = 67043328


def weights_of(lower, upper):
    return [(upper ** (k + 1) - lower ** (k + 1)) / math.factorial(k + 1) for k in range(ORDER)]


def dot(a, b):
    return jnp.dot(a, b, preferred_element_type=F32)


def split2(x):
    high = x.astype(BF16)
    return high, (x - high.astype(F32)).astype(BF16)


def split3(x):
    high = x.astype(BF16)
    rest = x - high.astype(F32)
    mid = rest.astype(BF16)
    return high, mid, (rest - mid.astype(F32)).astype(BF16)


def dot3(a, b, dims=None):
    total = None
    for part in split3(a):
        if dims is None:
            term = dot(part, b)
        else:
            term = lax.dot_general(part, b, (dims, ((), ())), preferred_element_type=F32)
        total = term if total is None else total + term
    return total


def dot2(a, b):
    high, low = split2(a)
    return dot(high, b) + dot(low, b)


def product(op, both):
    depth, width = both.shape[0], both.shape[1] // 2
    wide = dot(op[0:ROWS, 0:depth], both[...])
    return wide[:, 0:width] + wide[:, width:] + dot(op[ROWS:, 0:depth], both[:, 0:width])


def put(both, at, value):
    width = both.shape[1] // 2
    high, low = split2(value)
    both[ROWS * at : ROWS * (at + 1), 0:width] = high
    both[ROWS * at : ROWS * (at + 1), width:] = low


PATH = (0, 1, 2, 3, 7, 11, 15, 14, 10, 6, 5, 9, 13, 12, 8, 4)


def owner_of(device):
    group = device >> 3
    place = jnp.zeros_like(group)
    for k, g in enumerate(PATH):
        place = jnp.where(group == g, k, place)
    inner = device & 7
    return place * 8 + jnp.where((place & 1) > 0, inner ^ 6, inner)


def device_of(owner):
    group = owner // 8
    return PATH[group] * 8 + (owner % 8 ^ (6 if group % 2 else 0))


def iota(shape, dim):
    return lax.broadcasted_iota(jnp.int32, shape, dim)


def onehot(condition):
    return jnp.where(condition, 1.0, 0.0).astype(BF16)


def pack_rows(stage, out_ref):
    for k in range(8):
        out_ref[pl.ds(k, DEVS, stride=8), :] = stage[128 * k : 128 * k + 128, :].T


def unpack_rows(recv_ref, stage):
    for k in range(8):
        stage[128 * k : 128 * k + 128, :] = recv_ref[pl.ds(k, DEVS, stride=8), :].T


def scatter_kernel(
    core, modal, jac, area, cluster, target, faces, listed, out, tables, cells, values, stage, kinds, places, lists, done
):
    copies = [
        pltpu.make_async_copy(modal, cells, done.at[0]),
        pltpu.make_async_copy(jac, values.at[0:3, :], done.at[1]),
        pltpu.make_async_copy(area, values.at[3:7, :], done.at[2]),
        pltpu.make_async_copy(cluster, kinds, done.at[3]),
        pltpu.make_async_copy(target, places, done.at[4]),
        pltpu.make_async_copy(faces, tables.at[0:4, :], done.at[5]),
        pltpu.make_async_copy(listed, lists, done.at[6]),
    ]
    for copy in copies:
        copy.start()
    copies[4].wait()
    half = owner_of(iota((DEVS, DEVS), 0)) * CAP
    slot = jnp.concatenate([half, half], axis=1)
    wanted = places[...]
    hots = [onehot(slot + t == wanted) for t in range(CAP)]
    tables[8:16, :] = jnp.zeros((8, SLOTS), jnp.int32)
    values[320:328, :] = jnp.zeros((8, BLOCK), F32)
    stage[CAP * STRIDE :, :] = jnp.zeros((CHUNK - CAP * STRIDE, DEVS), F32)
    for t in range(CAP):
        stage[STRIDE * t + 328 : STRIDE * (t + 1), :] = jnp.zeros((8, DEVS), F32)
    for k in (0, 1, 2, 3, 5, 6):
        copies[k].wait()
    tables[4:8, :] = jnp.full((4, SLOTS), core[0], jnp.int32)
    for i in range(GHOSTS):
        tables[8 + i : 9 + i, 0:NEIGH] = lists[i]
    values[7:8, :] = 1.0 + kinds[...].astype(F32)
    for q in range(QUANT):
        values[8 + MODES * q : 8 + MODES * (q + 1), :] = cells[q]
    parts = split3(values[...])
    for t in range(CAP):
        total = None
        for part in parts:
            term = lax.dot_general(part, hots[t], (((1,), (1,)), ((), ())), preferred_element_type=F32)
            total = term if total is None else total + term
        stage[STRIDE * t : STRIDE * t + 328, :] = total
    pack_rows(stage, out)


def gather_kernel(recv, target, out, stage):
    unpack_rows(recv, stage)
    wanted = target[...]
    half = owner_of(iota((DEVS, DEVS), 0)) * CAP
    slot = jnp.concatenate([half, half], axis=1)
    held = jnp.concatenate([stage[STRIDE * t + 8 : STRIDE * t + 8 + ROWS, :] for t in range(CAP)], axis=1)
    total = dot3(held, jnp.concatenate([onehot(slot + t == wanted) for t in range(CAP)], axis=0))
    for q in range(QUANT):
        out[q] = total[MODES * q : MODES * (q + 1), :]


def pair_codes():
    col = iota((8, 2 * ROWS), 1)
    second = jnp.where(col >= ROWS, 1, 0)
    inner = col - second * ROWS
    quant = (inner * 1873) >> 16
    mode = inner - quant * MODES
    valid = inner < FEAT
    mode_code = jnp.where(valid, second * 128 + mode, -1)[0:1]
    quant_code = jnp.where(valid, second * 16 + quant, -512)[0:1]
    row = iota((256, 2 * ROWS), 0)
    return row, onehot(row == mode_code), quant_code


def expand_pairs(first, last, count, tiles, columns, codes, stage, op, ready):
    row, mode_hot, quant_code = codes
    flux = split2(jnp.concatenate([columns[0:128, :].T[0:16, :], columns[128:256, :].T[0:16, :]], axis=1))
    for k in range(0, count, 2):
        width = ROWS * min(2, count - k)
        at = first + k
        pair = split2(jnp.concatenate([tiles[at], tiles[min(at + 1, last)]], axis=1))
        quant_hot = onehot(row == quant_code + 16 * at)
        spread = dot(pair[0], mode_hot) + dot(pair[1], mode_hot)
        scale = dot(flux[0], quant_hot) + dot(flux[1], quant_hot)
        for p in range(QUANT):
            stage[MODES * p : MODES * (p + 1), 0:width] = spread[0:MODES, 0:width] * scale[p : p + 1, 0:width]
        high, low = split2(stage[:, 0:width])
        op[0:ROWS, ROWS * k : ROWS * k + width] = high
        op[ROWS:, ROWS * k : ROWS * k + width] = low
        ready(slice(ROWS * k, ROWS * k + -(-width // 128) * 128))


def taylor_operator_kernel(stiffness, star, op, tiles, square, columns, stage):
    tiles[...] = jnp.zeros(tiles.shape, F32)
    square[...] = jnp.zeros(square.shape, F32)
    columns[...] = jnp.zeros(columns.shape, F32)
    stage[FEAT:ROWS, :] = jnp.zeros((ROWS - FEAT, stage.shape[1]), F32)
    for c in range(3):
        square[0:MODES, 0:MODES] = -stiffness[c]
        tiles[c] = square[...].T[0:48, :]
        columns[16 * c : 16 * c + QUANT, 0:QUANT] = star[:, c, :]
    expand_pairs(0, 2, 3, tiles, columns, pair_codes(), stage, op, lambda lanes: None)


def operator_kernel(
    stiffness, minus, plus, star, solver_minus, solver_plus, c_out, b_out,
    k_in, m_in, p_in, s_in, sm_in, sp_in, tiles, columns, stage, c_op, b_op, loads, done,
):
    copies = fetch(
        [
            (stiffness, k_in), (minus, m_in), (plus, p_in), (star, s_in),
            (solver_minus, sm_in), (solver_plus, sp_in),
        ],
        loads,
    )
    codes = pair_codes()
    tiles[...] = jnp.zeros(tiles.shape, F32)
    columns[...] = jnp.zeros(columns.shape, F32)
    stage[FEAT:ROWS, :] = jnp.zeros((ROWS - FEAT, stage.shape[1]), F32)
    for copy in copies:
        copy.wait()
    for c in range(3):
        tiles[c, 0:MODES, 0:MODES] = k_in[c]
        columns[16 * c : 16 * c + QUANT, 0:QUANT] = s_in[:, c, :]
    for f in range(4):
        tiles[3 + f, 0:MODES, 0:MODES] = -m_in[:, f, :]
        tiles[7 + f, 0:MODES, 0:MODES] = -p_in[:, f, :]
        columns[16 * (3 + f) : 16 * (3 + f) + QUANT, 0:QUANT] = sm_in[:, f, :]
        columns[16 * (7 + f) : 16 * (7 + f) + QUANT, 0:QUANT] = sp_in[:, f, :]
    sent = []

    def leave(op, out):
        return lambda lanes: sent.extend(fetch([(op.at[:, lanes], out.at[:, lanes])], done, len(sent)))

    expand_pairs(0, 10, 7, tiles, columns, codes, stage, c_op, leave(c_op, c_out))
    expand_pairs(7, 10, 4, tiles, columns, codes, stage, b_op, leave(b_op, b_out))
    for copy in sent:
        copy.wait()


def order_faces(faces):
    digits = jnp.concatenate([faces >> 4, faces & 15], axis=0).astype(F32).astype(BF16)
    from_slot = iota((SLOTS, SLOTS), 0)
    to_slot = iota((SLOTS, SLOTS), 1)
    moved = dot(digits, onehot(from_slot == (to_slot & 127) * CAP + (to_slot >> 7))).astype(jnp.int32)
    return moved[0:4, :] * 16 + moved[4:8, :]


def taylor(start, extras, d_op, pieces, factor_sets):
    cuts = [(0, 256), (256, SLOTS)]
    current = [start[:, lo:hi] for lo, hi in cuts]
    sums = [[value * factors[0] for value in current] for factors in factor_sets]
    for k in range(1, ORDER):
        for i, (lo, hi) in enumerate(cuts):
            for c in range(3):
                put(pieces[i], c, current[i] * extras[c : c + 1, lo:hi])
            current[i] = product(d_op, pieces[i])
            for total, factors in zip(sums, factor_sets):
                total[i] = total[i] + current[i] * factors[k]
    return [jnp.concatenate(total, axis=1) for total in sums]


def order_picks(listed, picks):
    value = listed
    digits = jnp.concatenate([value >> 4, value & 15], axis=0).astype(F32).astype(BF16)
    spread = dot(digits, onehot(iota((128, 128), 0) == (iota((128, 128), 1) >> 3))).astype(jnp.int32)
    spread = spread[0:8, :] * 16 + spread[8:16, :]
    lane = iota((1, 128), 1)
    part = jnp.where(lane < 64, lane & 7, 8)

    def choose(*moves):
        line = jnp.full((1, 128), -1, jnp.int32)
        for ghost, spot in moves:
            line = jnp.where(part == spot, spread[ghost : ghost + 1, :], line)
        return line

    picks[...] = jnp.full(picks.shape, -1, jnp.int32)
    picks[0:1, :] = choose(*[(i, i) for i in range(GHOSTS)])
    picks[1:2, :] = choose((0, 6), (2, 7))
    picks[2:3, :] = choose((1, 6), (3, 7))
    picks[3:4, :] = choose((4, 6))
    picks[4:5, :] = choose((5, 6))


def send_ghosts(value, picks, odd, even):
    slot = iota((SLOTS, 128), 0)
    slot = (slot & 127) * CAP + (slot >> 7)
    base = onehot(slot == picks[0:1, :])
    rest = jnp.concatenate([onehot(slot == picks[k : k + 1, :]) for k in range(1, 5)], axis=1)
    main = dot2(value[0:256, :], base)
    tail = dot2(value[256:320, :], rest)
    first = (main[0:128, :] + jnp.concatenate([tail[:, 0:128], tail[:, 128:256]], axis=0)).T
    second = (main[128:256, :] + jnp.concatenate([tail[:, 256:384], tail[:, 384:512]], axis=0)).T
    for b, step in enumerate(STEPS):
        out = odd if step % 2 else even
        place = 16 * (SENT.index(step) % 4)
        out[place : place + 8, :] = first[8 * b : 8 * b + 8, :]
        out[place + 8 : place + 16, :] = second[8 * b : 8 * b + 8, :]


def relay_kernel(even, twin, up, down, far_up, far_down):
    def piece(rows, step):
        place = 16 * (SENT.index(step) % 4)
        return rows[place : place + 16, :]

    for out, sign in ((up, 1), (down, -1)):
        out[0:16, :] = piece(even, 2 * sign)
        out[16:32, :] = piece(twin, sign)
        out[32:48, :] = piece(twin, 3 * sign)
    for out, sign in ((far_up, 1), (far_down, -1)):
        out[0:16, :] = piece(even, 4 * sign)
        out[16:32, :] = piece(twin, 3 * sign)


def read_ghosts(twin, up, down, far_up, far_down, core):
    even = core == 0
    places = {
        2: (up, 0, up, 0), -2: (down, 0, down, 0), 4: (far_up, 0, far_up, 0), -4: (far_down, 0, far_down, 0),
        1: (up, 16, twin, 0), -1: (twin, 16, down, 16), 3: (far_up, 16, up, 32), -3: (down, 32, far_down, 16),
    }
    firsts, seconds = [], []
    for step in STEPS:
        a, i, b, j = places[step]
        firsts.append(jnp.where(even, a[i : i + 8, :], b[j : j + 8, :]))
        seconds.append(jnp.where(even, a[i + 8 : i + 16, :], b[j + 8 : j + 16, :]))
    blank = jnp.zeros((64, 128), F32)
    first = jnp.concatenate(firsts + [blank], axis=0).T
    second = jnp.concatenate(seconds + [blank], axis=0).T
    row = iota((128, 128), 0)
    col = iota((128, 128), 1)
    part = col & 7
    group = col - part
    halves = [first[0:64, :], first[64:128, :], second[0:64, :], second[64:128, :]]
    places = [((0, 6), (2, 7)), ((1, 6), (3, 7)), ((4, 6),), ((5, 6),)]
    tail = None
    for half, moves in zip(halves, places):
        hit = None
        for ghost, spot in moves:
            one = (part == ghost) & (row == group + spot)
            hit = one if hit is None else hit | one
        term = dot2(half, onehot(hit))
        tail = term if tail is None else tail + term
    return jnp.concatenate([first, second, tail], axis=0)


def remote_flux(value, ghosts, extras, faces, b_op, both):
    high, low = split2(jnp.concatenate([value, ghosts], axis=1))
    row = iota((512, 128), 0)
    beyond = row - SLOTS
    local = (row & 127) * CAP + (row >> 7)
    spot = beyond & 7
    ghost = jnp.where((spot < GHOSTS) & (beyond < 64), SLOTS + (beyond >> 3) * GHOSTS + spot, -1)
    code = jnp.where(row < SLOTS, local, ghost)
    for f in range(4):
        hot = jnp.concatenate(
            [onehot(code == faces[f : f + 1, 128 * k : 128 * (k + 1)]) for k in range(3)], axis=1
        )
        picked = (dot(high, hot) + dot(low, hot)) * extras[3 + f : 4 + f, :]
        put(both, f, picked)
    return product(b_op, both)


def fetch(pairs, done, base=0):
    copies = [pltpu.make_async_copy(src, dst, done.at[base + k]) for k, (src, dst) in enumerate(pairs)]
    for copy in copies:
        copy.start()
    return copies


def occupied(extras):
    return jnp.where(extras[7:8, :] > 0.5, 1.0, 0.0)


def unpack_kernel(recv, tables, state, extras, picks, stage):
    order_picks(tables[8:16, 0:128], picks)
    unpack_rows(recv, stage)
    for t in range(CAP):
        extras[:, 128 * t : 128 * (t + 1)] = stage[STRIDE * t : STRIDE * t + 8, :]
        state[:, 128 * t : 128 * (t + 1)] = stage[STRIDE * t + 8 : STRIDE * t + 8 + ROWS, :]


def start_kernel(state, extras, picks, d_op, first, later, odd, even, one_piece, other_piece):
    one, two = taylor(
        state[...], extras, d_op, (one_piece, other_piece), [weights_of(0.0, 1.0), weights_of(1.0, 2.0)]
    )
    first[...] = one
    later[...] = two
    send_ghosts(first, picks, odd, even)


def local_kernel(state, value, extras, c_op, faces, out, order, both):
    order[...] = order_faces(faces[0:4, :])
    local_terms(state, value, extras, c_op, out, both)


def local_terms(state, value, extras, c_op, out, both):
    for k in range(7):
        put(both, k, value[...] * extras[k : k + 1, :])
    change = product(c_op, both)
    out[...] = state[...] + occupied(extras) * change


def middle_kernel(
    core, twin, up, down, far_up, far_down, partial, first, later, extras, faces, picks, d_op, b_op,
    middle, second, odd, even, one_piece, other_piece, wide,
):
    table = read_ghosts(twin, up, down, far_up, far_down, core[0])
    flux = remote_flux(first[...], table, extras, faces, b_op, wide)
    middle[...] = partial[...] + occupied(extras) * flux
    (fresh,) = taylor(middle[...], extras, d_op, (one_piece, other_piece), [weights_of(0.0, 1.0)])
    second[...] = jnp.where(extras[7:8, :] > 1.5, later[...], fresh)
    send_ghosts(second, picks, odd, even)


def final_kernel(
    core, twin, up, down, far_up, far_down, partial, second, extras, faces, b_op, out, stage, wide
):
    table = read_ghosts(twin, up, down, far_up, far_down, core[0])
    flux = remote_flux(second[...], table, extras, faces, b_op, wide)
    final = partial[...] + occupied(extras) * flux
    stage[...] = jnp.zeros((CHUNK, DEVS), F32)
    for t in range(CAP):
        stage[STRIDE * t + 8 : STRIDE * t + 8 + ROWS, :] = final[:, 128 * t : 128 * (t + 1)]
    pack_rows(stage, out)


def shape(*dims, dtype=F32):
    return jax.ShapeDtypeStruct(dims, dtype)


def call(kernel, name, outs, scratch, flops, operands, spaces="", out_spaces="", limit=16 * 1024 * 1024):
    kinds = {"s": pltpu.SMEM, "v": pltpu.VMEM, "h": pltpu.HBM}
    spaces = spaces.ljust(len(operands), "v")
    flat = jax.tree.leaves(outs)
    out_specs = [pl.BlockSpec(memory_space=kinds[k]) for k in out_spaces.ljust(len(flat), "v")]
    moved = sum(math.prod(o.shape) * 4 for o in operands)
    return pl.pallas_call(
        kernel,
        name=name,
        out_shape=outs,
        in_specs=[pl.BlockSpec(memory_space=kinds[k]) for k in spaces],
        out_specs=out_specs if isinstance(outs, list) else out_specs[0],
        scratch_shapes=scratch,
        cost_estimate=pl.CostEstimate(flops=flops, bytes_accessed=moved, transcendentals=0),
        compiler_params=pltpu.CompilerParams(vmem_limit_bytes=limit),
    )(*operands)


def vmem(*dims, dtype=F32):
    return pltpu.VMEM(dims, dtype)


def exchange(rows, per):
    cube = rows.reshape(DEVS, per, 128)
    return lax.all_to_all(cube, "dom", split_axis=0, concat_axis=0, tiled=True).reshape(DEVS * per, 128)


def swap_ghosts(odd, even, value):
    def move(part, shift):
        pairs = [(device_of(o), device_of((o + shift) % DEVS)) for o in range(DEVS)]
        return lax.ppermute(part, "dom", pairs)

    twins = [(device_of(o), device_of(o ^ 1)) for o in range(DEVS)]
    twin = lax.ppermute(odd, "dom", twins)
    parts = call(
        relay_kernel, "relay", [shape(48, 128), shape(48, 128), shape(32, 128), shape(32, 128)], [], 10**6, (even, twin)
    )
    value, parts = lax.optimization_barrier((value, parts))
    return (twin, *[move(part, shift) for part, shift in zip(parts, (2, -2, 4, -4))]), value


def local(
    modal_dofs, jacobian, face_area, cluster_id, target_slot, ghost_slots, face_neighbours,
    stiffness, star_matrix, face_minus, face_plus, solver_minus, solver_plus,
):
    core = (lax.axis_index("dom").astype(jnp.int32) & 1).reshape(1)
    target = target_slot.reshape(1, BLOCK)
    sent, tables = call(
        scatter_kernel, "scatter", [shape(CHUNK, DEVS), shape(16, SLOTS, dtype=jnp.int32)],
        [
            vmem(QUANT, MODES, BLOCK), vmem(328, BLOCK), vmem(CHUNK, DEVS), vmem(1, BLOCK, dtype=jnp.int32),
            vmem(1, BLOCK, dtype=jnp.int32), vmem(6, 1, NEIGH, dtype=jnp.int32), pltpu.SemaphoreType.DMA((7,)),
        ],
        10**8,
        (
            core, jnp.transpose(modal_dofs, (1, 0, 2)), jacobian, face_area, cluster_id.reshape(1, BLOCK), target,
            face_neighbours, jnp.transpose(ghost_slots, (2, 0, 1)),
        ),
        "shhhhhhh", "", FULL,
    )
    received = exchange(sent, 8)

    star, minus, plus, solve_minus, solve_plus = [
        jnp.transpose(a, (1, 0, 2)) for a in (star_matrix, face_minus, face_plus, solver_minus, solver_plus)
    ]
    c_op, b_op = call(
        operator_kernel, "operators",
        [shape(2 * ROWS, w, dtype=BF16) for w in (2304, 1280)],
        [
            vmem(3, MODES, MODES), vmem(MODES, 4, MODES), vmem(MODES, 4, MODES),
            vmem(QUANT, 3, QUANT), vmem(QUANT, 4, QUANT), vmem(QUANT, 4, QUANT),
            vmem(11, 48, 128), vmem(256, 128), vmem(ROWS, 2 * ROWS), vmem(2 * ROWS, 2304, dtype=BF16),
            vmem(2 * ROWS, 1280, dtype=BF16), pltpu.SemaphoreType.DMA((6,)), pltpu.SemaphoreType.DMA((6,)),
        ],
        10**9, (stiffness, minus, plus, star, solve_minus, solve_plus), "hhhhhh", "hh", FULL - 1900 * 1024,
    )
    stiffness, star, _ = lax.optimization_barrier((stiffness, star, b_op))
    d_op = call(
        taylor_operator_kernel, "taylor_operators", shape(2 * ROWS, 960, dtype=BF16),
        [vmem(3, 48, 128), vmem(128, 128), vmem(256, 128), vmem(ROWS, 2 * ROWS)],
        10**9, (stiffness, star),
    )
    home = [(o, device_of(o)) for o in range(DEVS)]
    tables = lax.ppermute(tables, "dom", home)
    received, tables = lax.optimization_barrier((received, tables))
    x_scratch = [vmem(3 * ROWS, 512, dtype=BF16), vmem(3 * ROWS, 256, dtype=BF16)]
    y_scratch = [vmem(4 * ROWS, 2 * SLOTS, dtype=BF16)]
    z_scratch = [vmem(7 * ROWS, 2 * SLOTS, dtype=BF16)]
    field = shape(ROWS, SLOTS)
    halo = [shape(64, 128)] * 2
    state, extras, picks = call(
        unpack_kernel, "unpack", [field, shape(8, SLOTS), shape(8, 128, dtype=jnp.int32)],
        [vmem(CHUNK, DEVS)], 10**8, (received, tables),
    )
    first, later, odd, even = call(
        start_kernel, "start", [field, field, *halo], x_scratch, 10**9, (state, extras, picks, d_op),
    )
    ghosts, first = swap_ghosts(odd, even, first)
    partial1, faces = call(
        local_kernel, "local1", [field, shape(4, SLOTS, dtype=jnp.int32)], z_scratch, 10**9,
        (state, first, extras, c_op, tables),
    )
    middle, second, odd, even = call(
        middle_kernel, "middle", [field, field, *halo],
        x_scratch + y_scratch, 2 * 10**9,
        (core, *ghosts, partial1, first, later, extras, faces, picks, d_op, b_op), "s",
    )
    ghosts, second = swap_ghosts(odd, even, second)
    partial2 = call(
        local_terms, "local2", field, z_scratch, 10**9, (middle, second, extras, c_op)
    )
    back = call(
        final_kernel, "final", shape(CHUNK, DEVS),
        [vmem(CHUNK, DEVS)] + y_scratch, 10**9,
        (core, *ghosts, partial2, second, extras, faces, b_op), "s",
    )
    returned = exchange(back, 8)
    result = call(
        gather_kernel, "gather", shape(QUANT, MODES, BLOCK), [vmem(CHUNK, DEVS)], 10**8, (returned, target)
    )
    return jnp.transpose(result, (1, 0, 2))


def solution(mesh):
    placed = (
        P(None, None, "dom"), P(None, "dom"), P(None, "dom"), P("dom"), P("dom"), P("dom", None, None),
        P(None, "dom"), P(), P(), P(), P(), P(), P(),
    )
    return jax.shard_map(
        local, mesh=mesh, in_specs=placed, out_specs=P(None, None, "dom"), check_vma=False
    )
```
